128 devices in a mesh: member: 16 (over z, x_lo, core), space: 8 (over x_hi, y).
Axes of the slice: x: 4 (x_hi: 2, x_lo: 2; x = x_hi * 2 + x_lo), y: 4, z: 4, core: 2. Of those that a mesh axis runs over, the one named last changes fastest.
Arguments:
- weather: bfloat16 [16, 84, 256, 1440], P('member', None, 'space'), may hold values from -6 to 6
- coefficients: int32 [16, 84, 2, 368, 361], P('member', None, None, 'space'), may hold values from -1073741824 to 1073741823
- channel_scale: float32 [84], replicated, may hold values from 0.3 to 3
Outputs:
- perturbed: bfloat16 [16, 84, 256, 1440], P('member', None, 'space')
The draws below stay inside these ranges and needn't reach their ends.
All inputs are finite; a program needn't handle non-finite values.
Results may differ from the reference program's by a relative error of at most 0.007.
Values may be sent and summed in bfloat16 or wider, within the bound.
A program may use at most 192 MiB of HBM per device.

```python
import math
import jax
import jax.numpy as jnp
from jax import lax

CH = 84
LON = 1440
E = 16
LAT = 256
LAT0 = 232
LP = 361
MP = 368


def with_ends(values, rng, low, largest):
    longest = values.shape.index(max(values.shape))
    spots = []
    for shift in (0, 1):
        where = [jax.random.randint(jax.random.fold_in(rng, axis), (), 0, length) for axis, length in enumerate(values.shape)]
        where[longest] = (where[longest] + shift) % values.shape[longest]
        spots.append(tuple(where))
    return values.at[spots[0]].set(low).at[spots[1]].set(largest)


def shard_levels(key, extent, pieces, least, high):
    level = 1.0
    for position, blocks in pieces:
        heights = jax.random.uniform(jax.random.fold_in(jax.random.fold_in(key, 6), position), (blocks,), jnp.float32, least / len(pieces), high / len(pieces))
        level = level * jnp.repeat(jnp.exp(heights), extent[position] // blocks).reshape((-1,) + (1,) * (len(extent) - 1 - position))
    return level


def normal_values(own_key, dims, spread, reach, shards=(), kind=jnp.bfloat16):
    loudness = shard_levels(own_key, dims, shards, -0.22, 0.18) if shards else 1.0
    values = jax.random.normal(own_key, dims, jnp.float32) * spread * loudness
    return jnp.minimum(jnp.maximum(values, -reach), reach).astype(kind)


def setup_inputs(seed: int = 0) -> dict:
    key_list = jax.random.split(jax.random.key(seed), 4)
    weather = normal_values(key_list[0], (E, CH, LAT, LON), 1.0, 6.0, ((0, 16), (2, 8)))
    coefficients = with_ends(jax.random.randint(key_list[1], (E, CH, 2, MP, LP), -1073741824, 1073741824), jax.random.fold_in(key_list[1], 1), -1073741824, 1073741823).astype(jnp.int32)
    channel_scale = jnp.clip(jnp.exp(jax.random.uniform(key_list[2], (CH,), jnp.float32, math.log(0.3), math.log(3.0))), 0.3, 3.0)
    return dict(weather=weather, coefficients=coefficients, channel_scale=channel_scale)


def diagonal_log(order_count):
    steps_up = jnp.arange(1, order_count, dtype=jnp.int32).astype(jnp.float32)
    terms = 0.5 * jnp.log((2.0 * steps_up + 1.0) / (2.0 * steps_up))
    return jnp.concatenate([jnp.zeros((1,), jnp.float32), jnp.cumsum(terms)])

def legendre_table(orders, colatitude, order_logs, degree_count):
    order_values = orders.astype(jnp.float32)[:, None]
    cosine = jnp.cos(colatitude)[None, :]
    sine_values = jnp.sin(colatitude)[None, :]
    diagonal = jnp.exp(order_logs[:, None] - 0.5 * math.log(4.0 * math.pi) + order_values * jnp.log(sine_values))
    block_size = 16
    turn_count = (degree_count + block_size - 1) // block_size
    order_square = order_values * order_values

    def advance(carry, turn_index):
        older_row, newer_row = carry
        produced = []
        for inner_step in range(block_size):
            degree = (turn_index * block_size + inner_step).astype(jnp.float32)
            degree_square = degree * degree
            prior = degree - 1.0
            factor_up = jnp.sqrt(jnp.maximum(4.0 * degree_square - 1.0, 1.0) / jnp.maximum(degree_square - order_square, 1.0))
            factor_down = jnp.sqrt(jnp.maximum(prior * prior - order_square, 0.0) / jnp.maximum(4.0 * prior * prior - 1.0, 1.0))
            next_row = factor_up * (cosine * newer_row - factor_down * older_row)
            next_row = jnp.where(degree < order_values, 0.0, jnp.where(degree == order_values, diagonal, next_row))
            produced.append(next_row)
            older_row, newer_row = (newer_row, next_row)
        return ((older_row, newer_row), jnp.stack(produced))
    empty = jnp.zeros_like(diagonal)
    carried, stacked = lax.scan(advance, (empty, empty), jnp.arange(turn_count, dtype=jnp.int32))
    return stacked.reshape(turn_count * block_size, orders.shape[0], colatitude.shape[0])[:degree_count]

def spectral_values(coefficients, orders):
    degree_count = coefficients.shape[-1]
    degrees = jnp.arange(degree_count, dtype=jnp.int32)
    keep = degrees[None, :] >= orders[:, None]
    factor = math.sqrt(3.0) * math.sqrt(4.0 * math.pi) / degree_count * 2.0 ** (-30)
    values = coefficients.astype(jnp.float32) * factor
    return jnp.where(keep, values, 0.0).astype(jnp.bfloat16)

def fourier_basis(order_count, lon_count):
    orders = jnp.arange(order_count, dtype=jnp.int32)
    columns = jnp.arange(lon_count, dtype=jnp.int32)
    phases = orders[:, None] * columns[None, :] % lon_count
    angles = 2.0 * math.pi / lon_count * phases.astype(jnp.float32)
    weights = jnp.where(orders == 0, 1.0, math.sqrt(2.0)).astype(jnp.float32)[:, None]
    return jnp.stack([weights * jnp.cos(angles), weights * jnp.sin(angles)]).astype(jnp.bfloat16)

def reference(weather, coefficients, channel_scale):
    orders = jnp.arange(MP, dtype=jnp.int32)
    colatitude = math.pi * (LAT0 + jnp.arange(LAT, dtype=jnp.int32)).astype(jnp.float32) / (LON // 2)
    legendre = legendre_table(orders, colatitude, diagonal_log(MP), LP).astype(jnp.bfloat16)
    legendre_wide = lax.optimization_barrier(legendre).astype(jnp.float32)
    basis = fourier_basis(MP, LON).reshape(2 * MP, LON)

    def one_member(coef_member):
        spectral = lax.optimization_barrier(spectral_values(coef_member, orders)).astype(jnp.float32)
        fourier = jnp.einsum('cpml,lmt->ctpm', spectral, legendre_wide, precision=lax.Precision.HIGHEST).astype(jnp.bfloat16)
        noise = jnp.dot(fourier.reshape(CH * LAT, 2 * MP), basis, preferred_element_type=jnp.float32)
        return noise.astype(jnp.bfloat16).reshape(CH, LAT, LON)
    noise_all = lax.map(one_member, coefficients)

    def add_up(total, noise_member):
        return (total + noise_member.astype(jnp.float32), None)
    total, unused = lax.scan(add_up, jnp.zeros((CH, LAT, LON), jnp.float32), noise_all)
    mean = total / E

    def perturb(pair):
        weather_member, noise_member = pair
        centred = noise_member.astype(jnp.float32) - mean
        return (weather_member.astype(jnp.float32) + channel_scale[:, None, None] * centred).astype(jnp.bfloat16)
    return lax.map(perturb, (weather, noise_all))
```

```python
import functools
import math

import jax
import jax.numpy as jnp
from jax import lax
from jax.experimental import pallas as pl
from jax.experimental.pallas import tpu as pltpu
from jax.sharding import PartitionSpec as P

MESH = pl.DeviceIdType.MESH

CH = 84
LON = 1440
TCOUNT = 256
LP = 361
BANDS = 8
ORDERS = 46
CHUNKS = 2
ORDP = 24
Q = 4
R = CH // Q
RP = 24
MROWS = 2 * Q * RP
MP = MROWS + 8
LROWS = 392
GROUP = 2 * ORDP
ROWS = CHUNKS * R * GROUP
ROWSP = 2048
OWN = 128
FACTOR = math.sqrt(3.0) * math.sqrt(4.0 * math.pi) / LP * 2.0 ** (-30)


def diagonal_log(order_count):
    steps_up = jnp.arange(1, order_count, dtype=jnp.int32).astype(jnp.float32)
    terms = 0.5 * jnp.log((2.0 * steps_up + 1.0) / (2.0 * steps_up))
    return jnp.concatenate([jnp.zeros((1,), jnp.float32), jnp.cumsum(terms)])


def lane_blocks(values, lane):
    low = lane < 64

    def swap(a, b, width, mask):
        ra = pltpu.roll(a, 128 - width, 1)
        rb = pltpu.roll(b, width, 1)
        return jnp.where(mask, a, rb), jnp.where(mask, ra, b)

    v0, v1, v2, v3 = values
    a0, a2 = swap(v0, v2, 64, low)
    a1, a3 = swap(v1, v3, 64, low)
    even = (lane % 64) < 32
    b0, b1 = swap(a0, a1, 32, even)
    b2, b3 = swap(a2, a3, 32, even)
    return b0, b1, b2, b3


def transform_kernel(coef_ref, cos_ref, diag_ref, f_ref, coef_v, lhs_v, tab, stage, sems):
    space = lax.axis_index("space")
    loads = [
        pltpu.make_async_copy(
            coef_ref.at[0, pl.ds(q * R, R)], coef_v.at[pl.ds(q * R, R)], sems.at[q]
        )
        for q in range(Q)
    ]
    for load in loads:
        load.start()

    def clear_lhs(n, _):
        lhs_v[2, pl.ds(pl.multiple_of(n * MP, 8), MP), :] = jnp.zeros((MP, 128), jnp.float32)
        return 0

    lax.fori_loop(0, ORDP, clear_lhs, 0)

    def clear_table(i, _):
        for h in range(2):
            for at in range(LP // 8 * 8, 384, 8):
                tab[h, pl.ds(pl.multiple_of(i * LROWS + at, 8), 8), :] = jnp.zeros(
                    (8, 128), jnp.float32
                )
        return 0

    lax.fori_loop(0, ORDP, clear_table, 0)

    def table(k):
        first = space * ORDERS + k * ORDP
        order = (first + lax.broadcasted_iota(jnp.int32, (ORDP, 128), 0)).astype(jnp.float32)
        square = order * order
        order_wide = first + lax.broadcasted_iota(jnp.int32, (ORDP, TCOUNT), 0)
        cosine = jnp.broadcast_to(cos_ref[...], (ORDP, TCOUNT))
        diag = diag_ref[k]
        older = jnp.zeros((ORDP, TCOUNT), jnp.float32)
        newer = jnp.zeros((ORDP, TCOUNT), jnp.float32)
        for tile in range(3):
            degree = tile * 128 + lax.broadcasted_iota(jnp.int32, (ORDP, 128), 1)
            degree = degree.astype(jnp.float32)
            degree_square = degree * degree
            prior = degree - 1.0
            up = jnp.sqrt(
                jnp.maximum(4.0 * degree_square - 1.0, 1.0)
                / jnp.maximum(degree_square - square, 1.0)
            )
            down = jnp.sqrt(
                jnp.maximum(prior * prior - square, 0.0)
                / jnp.maximum(4.0 * prior * prior - 1.0, 1.0)
            )

            def block(j, carry, steps=8):
                older, newer, up, down = carry
                for u in range(steps):
                    deg = tile * 128 + j * 8 + u
                    nxt = up[:, u : u + 1] * (cosine * newer - down[:, u : u + 1] * older)
                    nxt = jnp.where(order_wide == deg, diag, nxt)
                    for b in range(ORDP // 8):
                        for h in range(2):
                            tab[h, pl.ds(b * 8 * LROWS + deg, 8, stride=LROWS), :] = nxt[
                                8 * b : 8 * b + 8, 128 * h : 128 * h + 128
                            ]
                    older, newer = newer, nxt
                return older, newer, pltpu.roll(up, 120, 1), pltpu.roll(down, 120, 1)

            count = min(16, (LP - 128 * tile) // 8)
            carry = lax.fori_loop(0, count, block, (older, newer, up, down))
            if tile == 2:
                block(count, carry, steps=LP % 8)
            older, newer = carry[:2]

    def arrange(k, q):
        def one(r, _):
            for i in range(min(ORDP, ORDERS - k * ORDP)):
                for t in range(3):
                    wide = min(128, LP - 128 * t)
                    raw = coef_v[q * R + r, k * ORDP + i, :, pl.ds(128 * t, wide)]
                    lhs_v[t, pl.ds(i * MP + q * 48 + r, 2, stride=RP), pl.ds(0, wide)] = (
                        raw.astype(jnp.float32) * FACTOR
                    )
            return 0

        lax.fori_loop(0, R, one, 0)

    lane = lax.broadcasted_iota(jnp.int32, (RP * 2, 128), 1)

    def orders_of(k):
        def one(i, _):
            row = pl.multiple_of(i * MP, 8)
            lhs = jnp.concatenate(
                [lhs_v[t, pl.ds(row, MROWS), :].astype(jnp.bfloat16) for t in range(3)], axis=1
            )
            row = pl.multiple_of(i * LROWS, 8)
            rhs = jnp.concatenate(
                [tab[h, pl.ds(row, 384), :].astype(jnp.bfloat16) for h in range(2)], axis=1
            )
            out = jnp.dot(lhs, rhs, preferred_element_type=jnp.float32)
            for h in range(2):
                parts = [
                    out[48 * q : 48 * q + 48, 128 * h : 128 * h + 128] for q in range(Q)
                ]
                for b, part in enumerate(lane_blocks(parts, lane)):
                    s = 4 * h + b
                    for a in range(6):
                        stage[pl.ds((s * 48 + 8 * a) * ORDP + i, 8, stride=ORDP), :] = part[
                            8 * a : 8 * a + 8
                        ]
            return 0

        lax.fori_loop(0, min(ORDP, ORDERS - k * ORDP), one, 0)

    def pack_of(k):
        def pack(n, _):
            s, r = n // R, n % R
            first = stage[pl.ds(pl.multiple_of((s * 48 + r) * ORDP, 8), ORDP), :]
            second = stage[pl.ds(pl.multiple_of((s * 48 + RP + r) * ORDP, 8), ORDP), :]
            both = jnp.concatenate([first, second], axis=0).astype(jnp.bfloat16)
            f_ref[s, pl.ds(pl.multiple_of((k * R + r) * GROUP, 16), GROUP), :] = both
            return 0

        lax.fori_loop(0, BANDS * R, pack, 0)

    def clear(n, _):
        for i in range(ORDERS - ORDP, ORDP):
            stage[pl.ds(n * 8 * ORDP + i, 8, stride=ORDP), :] = jnp.zeros(
                (8, 128), jnp.float32
            )
        return 0

    for s in range(BANDS):
        f_ref[s, pl.ds(ROWS, ROWSP - ROWS), :] = jnp.zeros((ROWSP - ROWS, 128), jnp.bfloat16)

    table(0)
    for q in range(Q):
        loads[q].wait()
        arrange(0, q)
    orders_of(0)
    pack_of(0)
    lax.fori_loop(0, BANDS * 48 // 8, clear, 0)
    table(1)
    for q in range(Q):
        arrange(1, q)
    orders_of(1)
    pack_of(1)


def transform(coefficients, cosine, diag):
    return pl.pallas_call(
        transform_kernel,
        name="transform",
        out_shape=jax.ShapeDtypeStruct((BANDS, ROWSP, 128), jnp.bfloat16),
        in_specs=[
            pl.BlockSpec(memory_space=pl.ANY),
            pl.BlockSpec(memory_space=pltpu.VMEM),
            pl.BlockSpec(memory_space=pltpu.VMEM),
        ],
        out_specs=pl.BlockSpec(memory_space=pltpu.VMEM),
        scratch_shapes=[
            pltpu.VMEM((CH, ORDERS, 2, LP), jnp.int32),
            pltpu.VMEM((3, ORDP * MP, 128), jnp.float32),
            pltpu.VMEM((2, ORDP * LROWS, 128), jnp.float32),
            pltpu.VMEM((BANDS * 48 * ORDP, 128), jnp.float32),
            pltpu.SemaphoreType.DMA((Q,)),
        ],
        compiler_params=pltpu.CompilerParams(vmem_limit_bytes=56 * 2**20),
    )(coefficients, cosine, diag)


def exchange_kernel(
    f_ref, out_ref, basis_ref,
    got, mean, buf_a, buf_b, buf_c, piece,
    raw_s, raw_r, sa, ra, sb, rb, sc, rc, sd, rd, se, re, sf, rf, sg, rg,
):
    member, space = lax.axis_index("member"), lax.axis_index("space")
    z, xl, core = member // 4, (member // 2) % 2, member % 2

    def member_of(z, xl, core):
        return (z * 2 + xl) * 2 + core

    z_peers = [member_of((z + d) % 4, xl, core) for d in (1, 2, 3)]
    x_peer = member_of(z, 1 - xl, core)
    c_peer = member_of(z, xl, 1 - core)
    s_peers = [(space + d) % BANDS for d in range(1, BANDS)]
    barrier = pltpu.get_barrier_semaphore()
    for peer in z_peers + [x_peer, c_peer]:
        pl.semaphore_signal(barrier, inc=1, device_id=(peer, space), device_id_type=MESH)
    for peer in s_peers:
        pl.semaphore_signal(barrier, inc=1, device_id=(member, peer), device_id_type=MESH)
    pl.semaphore_wait(barrier, 5 + BANDS - 1)

    def remote(src, dst, ss, rs, device):
        return pltpu.make_async_remote_copy(
            src_ref=src, dst_ref=dst, send_sem=ss, recv_sem=rs,
            device_id=device, device_id_type=MESH,
        )

    half = 8 * OWN
    mine = pl.multiple_of(core * half, 16)
    other = pl.multiple_of((1 - core) * half, 16)
    pair = remote(f_ref.at[:, pl.ds(other, half)], buf_a, sa, ra, (c_peer, space))
    pair.start()
    raws = []
    for d in range(1, BANDS):
        raws.append(
            remote(
                f_ref.at[(space + d) % BANDS], got.at[d],
                raw_s.at[d - 1], raw_r.at[d - 1], (member, (space + d) % BANDS),
            )
        )
        raws[-1].start()

    pair.wait()

    def add_pair(n, _):
        s, j = n // 8, n % 8
        at = pl.multiple_of(j * 128, 16)
        total = buf_a[s, pl.ds(at, 128), :].astype(jnp.float32) + f_ref[
            s, pl.ds(mine + at, 128), :
        ].astype(jnp.float32)
        buf_a[s, pl.ds(at, 128), :] = total.astype(jnp.bfloat16)
        return 0

    lax.fori_loop(0, BANDS * 8, add_pair, 0)
    zs = []
    for d in (1, 2, 3):
        at = pl.multiple_of(((z + d) % 4) * 256, 16)
        zs.append(
            remote(
                buf_a.at[:, pl.ds(at, 256)], buf_b.at[d - 1],
                sb.at[d - 1], rb.at[d - 1], (z_peers[d - 1], space),
            )
        )
        zs[-1].start()

    column = lax.broadcasted_iota(jnp.int32, (ORDP, LON), 1).astype(jnp.float32)
    index = lax.broadcasted_iota(jnp.int32, (ORDP, LON), 0)

    def basis_block(n, _):
        order = n // CHUNKS * ORDERS + n % CHUNKS * ORDP + index
        product = order.astype(jnp.float32) * column
        turns = jnp.floor((product + 0.5) * (1.0 / LON))
        phase = product - turns * LON
        angle = 2.0 * math.pi / LON * phase
        weight = jnp.where(order == 0, 1.0, math.sqrt(2.0))
        weight = jnp.where(n % CHUNKS * ORDP + index < ORDERS, weight, 0.0)
        both = jnp.concatenate([weight * jnp.cos(angle), weight * jnp.sin(angle)], axis=0)
        basis_ref[pl.ds(pl.multiple_of(n * GROUP, 16), GROUP), :] = both.astype(jnp.bfloat16)
        return 0

    lax.fori_loop(0, BANDS * CHUNKS, basis_block, 0)

    for copy in zs:
        copy.wait()
    own_z = pl.multiple_of(z * 256, 16)

    def add_four(n, _):
        s, j = n // 2, n % 2
        at = pl.multiple_of(j * 128, 16)
        total = buf_a[s, pl.ds(own_z + at, 128), :].astype(jnp.float32)
        for d in range(3):
            total += buf_b[d, s, pl.ds(at, 128), :].astype(jnp.float32)
        piece[s, pl.ds(at, 128), :] = total.astype(jnp.bfloat16)
        return 0

    lax.fori_loop(0, BANDS * 2, add_four, 0)
    x_mine = pl.multiple_of(xl * OWN, 16)
    x_other = pl.multiple_of((1 - xl) * OWN, 16)
    step_c = remote(piece.at[:, pl.ds(x_other, OWN)], buf_c, sc, rc, (x_peer, space))
    step_c.start()
    step_c.wait()

    def add_two(s, _):
        total = buf_c[s].astype(jnp.float32) + piece[s, pl.ds(x_mine, OWN), :].astype(
            jnp.float32
        )
        buf_c[s] = (total * (1.0 / 16.0)).astype(jnp.bfloat16)
        return 0

    lax.fori_loop(0, BANDS, add_two, 0)
    own_row = pl.multiple_of(core * half + z * 256 + xl * OWN, 16)
    ds = []
    for d in range(1, BANDS):
        ds.append(
            remote(
                buf_c.at[(space + d) % BANDS], mean.at[d, pl.ds(own_row, OWN)],
                sd.at[d - 1], rd.at[d - 1], (member, (space + d) % BANDS),
            )
        )
        ds[-1].start()
    mean[0, pl.ds(own_row, OWN), :] = buf_c[space]
    for copy in ds:
        copy.wait()
    step_e = remote(
        mean.at[:, pl.ds(own_row, OWN)], mean.at[:, pl.ds(own_row, OWN)], se, re,
        (x_peer, space),
    )
    step_e.start()
    step_e.wait()
    z_row = pl.multiple_of(core * half + z * 256, 16)
    fs = []
    for d in (1, 2, 3):
        fs.append(
            remote(
                mean.at[:, pl.ds(z_row, 256)], mean.at[:, pl.ds(z_row, 256)],
                sf.at[d - 1], rf.at[d - 1], (z_peers[d - 1], space),
            )
        )
        fs[-1].start()
    for copy in fs:
        copy.wait()
    step_g = remote(
        mean.at[:, pl.ds(mine, half)], mean.at[:, pl.ds(mine, half)], sg, rg, (c_peer, space)
    )
    step_g.start()
    step_g.wait()
    for copy in raws:
        copy.wait()

    def centre(n, _):
        s, j = n // 9, n % 9
        at = pl.multiple_of(j * 224, 16)
        d = (space + BANDS - s) % BANDS
        block = got[d, pl.ds(at, 224), :].astype(jnp.float32)
        block = block - mean[d, pl.ds(at, 224), :].astype(jnp.float32)
        out_ref[s, pl.ds(at, 224), :] = block.astype(jnp.bfloat16)
        return 0

    def own(j, _):
        at = pl.multiple_of(j * 224, 16)
        got[0, pl.ds(at, 224), :] = f_ref[space, pl.ds(at, 224), :]
        return 0

    lax.fori_loop(0, 9, own, 0)
    lax.fori_loop(0, BANDS * 9, centre, 0)


def exchange(fourier):
    block = (BANDS, ROWSP, 128)
    sem = pltpu.SemaphoreType.DMA
    bf = jnp.bfloat16
    return pl.pallas_call(
        exchange_kernel,
        name="exchange",
        out_shape=[
            jax.ShapeDtypeStruct((BANDS, ROWS, 128), bf),
            jax.ShapeDtypeStruct((BANDS * CHUNKS * GROUP, LON), bf),
        ],
        in_specs=[pl.BlockSpec(memory_space=pltpu.VMEM)],
        out_specs=[pl.BlockSpec(memory_space=pltpu.VMEM)] * 2,
        scratch_shapes=[
            pltpu.VMEM(block, bf),
            pltpu.VMEM(block, bf),
            pltpu.VMEM((BANDS, 8 * OWN, 128), bf),
            pltpu.VMEM((3, BANDS, 256, 128), bf),
            pltpu.VMEM((BANDS, OWN, 128), bf),
            pltpu.VMEM((BANDS, 256, 128), bf),
            sem((7,)), sem((7,)),
            sem, sem,
            sem((3,)), sem((3,)),
            sem, sem,
            sem((7,)), sem((7,)),
            sem, sem,
            sem((3,)), sem((3,)),
            sem, sem,
        ],
        compiler_params=pltpu.CompilerParams(
            collective_id=1, has_side_effects=True, vmem_limit_bytes=50 * 2**20
        ),
    )(fourier)


RB = 3


def synthesis_kernel(f_ref, basis_ref, scale_ref, weather_ref, out_ref):
    step = pl.program_id(0)
    rows = []
    for r in range(RB):
        x = f_ref[:, :, r].reshape(BANDS * CHUNKS * GROUP, 128)
        rows.append(x.T)
    lhs = jnp.concatenate(rows, axis=0)
    noise = jnp.dot(lhs, basis_ref[...], preferred_element_type=jnp.float32)
    for r in range(RB):
        for q in range(Q):
            scale = scale_ref[q * R + step * RB + r]
            at = (r * Q + q) * 32
            out_ref[0, q, r] = (
                weather_ref[0, q, r].astype(jnp.float32) + scale * noise[at : at + 32]
            ).astype(jnp.bfloat16)


def synthesis(fourier, basis, scale, weather):
    fourier = fourier.reshape(BANDS, CHUNKS, R, GROUP, 128)
    rows = weather.shape[2]
    weather = weather.reshape(1, Q, R, rows, LON)
    block = pl.BlockSpec((1, Q, RB, rows, LON), lambda i: (0, 0, i, 0, 0))
    out = pl.pallas_call(
        synthesis_kernel,
        name="synthesis",
        grid=(R // RB,),
        out_shape=jax.ShapeDtypeStruct(weather.shape, jnp.bfloat16),
        in_specs=[
            pl.BlockSpec((BANDS, CHUNKS, RB, GROUP, 128), lambda i: (0, 0, i, 0, 0)),
            pl.BlockSpec(basis.shape, lambda i: (0, 0)),
            pl.BlockSpec(memory_space=pltpu.SMEM),
            block,
        ],
        out_specs=block,
        compiler_params=pltpu.CompilerParams(
            dimension_semantics=("arbitrary",), vmem_limit_bytes=50 * 2**20
        ),
    )(fourier, basis, scale, weather)
    return out.reshape(1, CH, rows, LON)


def tables():
    order = lax.axis_index("space") * ORDERS + jnp.arange(CHUNKS)[:, None] * ORDP
    order = order + jnp.arange(ORDP)[None, :]
    logs = diagonal_log(BANDS * ORDERS + 2)[order]
    row_first = (LON // 2 + 1 - TCOUNT) // 2
    colatitude = (
        math.pi
        * (row_first + jnp.arange(TCOUNT, dtype=jnp.int32)).astype(jnp.float32)
        / (LON // 2)
    )
    diag = jnp.exp(
        logs[:, :, None]
        - 0.5 * math.log(4.0 * math.pi)
        + order.astype(jnp.float32)[:, :, None] * jnp.log(jnp.sin(colatitude))
    )
    return jnp.cos(colatitude)[None, :], diag


def local(weather, coefficients, channel_scale):
    cosine, diag = tables()
    fourier = transform(coefficients.transpose(0, 1, 3, 2, 4), cosine, diag)
    centred, basis = exchange(fourier)
    return synthesis(centred, basis, channel_scale, weather)


def solution(mesh):
    return jax.shard_map(
        local,
        mesh=mesh,
        in_specs=(P("member", None, "space", None), P("member", None, None, "space", None), P()),
        out_specs=P("member", None, "space", None),
        check_vma=False,
    )
```

```python
import functools
import math

import jax
import jax.numpy as jnp
from jax import lax
from jax.experimental import pallas as pl
from jax.experimental.pallas import tpu as pltpu
from jax.sharding import PartitionSpec as P

MESH = pl.DeviceIdType.MESH

CH = 84
LON = 1440
TCOUNT = 256
LP = 361
BANDS = 8
ORDERS = 46
CHUNKS = 2
ORDP = 24
Q = 4
R = CH // Q
RP = 24
MROWS = 2 * Q * RP
MP = MROWS + 8
LROWS = 392
GROUP = 2 * ORDP
PIECE = R * GROUP
PIECEP = 1024
OWN = 128
FACTOR = math.sqrt(3.0) * math.sqrt(4.0 * math.pi) / LP * 2.0 ** (-30)


def diagonal_log(order_count):
    steps_up = jnp.arange(1, order_count, dtype=jnp.int32).astype(jnp.float32)
    terms = 0.5 * jnp.log((2.0 * steps_up + 1.0) / (2.0 * steps_up))
    return jnp.concatenate([jnp.zeros((1,), jnp.float32), jnp.cumsum(terms)])


def lane_blocks(values, lane):
    low = lane < 64

    def swap(a, b, width, mask):
        ra = pltpu.roll(a, 128 - width, 1)
        rb = pltpu.roll(b, width, 1)
        return jnp.where(mask, a, rb), jnp.where(mask, ra, b)

    v0, v1, v2, v3 = values
    a0, a2 = swap(v0, v2, 64, low)
    a1, a3 = swap(v1, v3, 64, low)
    even = (lane % 64) < 32
    b0, b1 = swap(a0, a1, 32, even)
    b2, b3 = swap(a2, a3, 32, even)
    return b0, b1, b2, b3


def fourier_kernel(
    coef_ref, cos_ref, diag_ref, out_ref, basis_ref,
    coef_v, lhs_v, tab, stage, f, got, mean, buf_a, buf_b, buf_c, piece,
    sems, raw_s, raw_r, sa, ra, sb, rb, sc, rc, sd, rd, sf, rf, sg, rg,
):
    member, space = lax.axis_index("member"), lax.axis_index("space")
    z, xl, core = member // 4, (member // 2) % 2, member % 2

    def member_of(z, xl, core):
        return (z * 2 + xl) * 2 + core

    cuts = (0, 32, 64, CH)
    loads = [
        pltpu.make_async_copy(
            coef_ref.at[0, pl.ds(lo, hi - lo)], coef_v.at[pl.ds(lo, hi - lo)], sems.at[n]
        )
        for n, (lo, hi) in enumerate(zip(cuts[:-1], cuts[1:]))
    ]
    for load in loads:
        load.start()

    z_peers = [member_of((z + d) % 4, xl, core) for d in (1, 2, 3)]
    x_peer = member_of(z, 1 - xl, core)
    c_peer = member_of(z, xl, 1 - core)
    s_peers = [(space + d) % BANDS for d in range(1, BANDS)]
    barrier = pltpu.get_barrier_semaphore()
    for peer in z_peers + [x_peer, c_peer]:
        pl.semaphore_signal(barrier, inc=1, device_id=(peer, space), device_id_type=MESH)
    for peer in s_peers:
        pl.semaphore_signal(barrier, inc=1, device_id=(member, peer), device_id_type=MESH)

    def clear_lhs(n, _):
        lhs_v[2, pl.ds(pl.multiple_of(n * MP, 8), MP), :] = jnp.zeros((MP, 128), jnp.float32)
        for h in range(2):
            for at in range(LP // 8 * 8, 384, 8):
                tab[h, pl.ds(pl.multiple_of(n * LROWS + at, 8), 8), :] = jnp.zeros(
                    (8, 128), jnp.float32
                )
        return 0

    lax.fori_loop(0, ORDP, clear_lhs, 0)
    for k in range(CHUNKS):
        for s in range(BANDS):
            f[k, s, pl.ds(PIECE, PIECEP - PIECE), :] = jnp.zeros(
                (PIECEP - PIECE, 128), jnp.bfloat16
            )

    def arrange(k, c):
        base = c // R * 48 + c % R
        for i in range(min(ORDP, ORDERS - k * ORDP)):
            for t in range(3):
                wide = min(128, LP - 128 * t)
                raw = coef_v[c, k * ORDP + i, :, pl.ds(128 * t, wide)]
                lhs_v[t, pl.ds(i * MP + base, 2, stride=RP), pl.ds(0, wide)] = (
                    raw.astype(jnp.float32) * FACTOR
                )

    def table(k, ready):
        first = space * ORDERS + k * ORDP
        order = (first + lax.broadcasted_iota(jnp.int32, (ORDP, 128), 0)).astype(jnp.float32)
        square = order * order
        order_wide = first + lax.broadcasted_iota(jnp.int32, (ORDP, TCOUNT), 0)
        cosine = jnp.broadcast_to(cos_ref[...], (ORDP, TCOUNT))
        diag = diag_ref[k]
        older = jnp.zeros((ORDP, TCOUNT), jnp.float32)
        newer = jnp.zeros((ORDP, TCOUNT), jnp.float32)
        for tile in range(3):
            degree = tile * 128 + lax.broadcasted_iota(jnp.int32, (ORDP, 128), 1)
            degree = degree.astype(jnp.float32)
            degree_square = degree * degree
            prior = degree - 1.0
            up = jnp.sqrt(
                jnp.maximum(4.0 * degree_square - 1.0, 1.0)
                / jnp.maximum(degree_square - square, 1.0)
            )
            down = jnp.sqrt(
                jnp.maximum(prior * prior - square, 0.0)
                / jnp.maximum(4.0 * prior * prior - 1.0, 1.0)
            )

            def block(j, carry, steps=8, channels=True):
                older, newer, up, down = carry
                for u in range(steps):
                    deg = tile * 128 + j * 8 + u
                    nxt = up[:, u : u + 1] * (cosine * newer - down[:, u : u + 1] * older)
                    nxt = jnp.where(order_wide == deg, diag, nxt)
                    for b in range(ORDP // 8):
                        for h in range(2):
                            tab[h, pl.ds(b * 8 * LROWS + deg, 8, stride=LROWS), :] = nxt[
                                8 * b : 8 * b + 8, 128 * h : 128 * h + 128
                            ]
                    older, newer = newer, nxt
                if channels:
                    for n in range(2):
                        arrange(k, tile * 32 + j * 2 + n)
                return older, newer, pltpu.roll(up, 120, 1), pltpu.roll(down, 120, 1)

            if not ready:
                loads[tile].wait()
            whole = (cuts[tile + 1] - cuts[tile]) // 2
            carry = lax.fori_loop(0, whole, block, (older, newer, up, down))
            if tile == 2:
                count = (LP - 128 * tile) // 8
                carry = lax.fori_loop(
                    whole, count, functools.partial(block, channels=False), carry
                )
                block(count, carry, steps=LP % 8, channels=False)
            older, newer = carry[:2]

    lane = lax.broadcasted_iota(jnp.int32, (RP * 2, 128), 1)

    def orders_of(k):
        def one(n, _):
            for i in (2 * n, 2 * n + 1):
                row = pl.multiple_of(i * MP, 8)
                lhs = jnp.concatenate(
                    [lhs_v[t, pl.ds(row, MROWS), :].astype(jnp.bfloat16) for t in range(3)],
                    axis=1,
                )
                row = pl.multiple_of(i * LROWS, 8)
                rhs = jnp.concatenate(
                    [tab[h, pl.ds(row, 384), :].astype(jnp.bfloat16) for h in range(2)], axis=1
                )
                out = jnp.dot(lhs, rhs, preferred_element_type=jnp.float32)
                for h in range(2):
                    parts = [
                        out[48 * q : 48 * q + 48, 128 * h : 128 * h + 128] for q in range(Q)
                    ]
                    for b, part in enumerate(lane_blocks(parts, lane)):
                        s = 4 * h + b
                        for a in range(6):
                            stage[
                                pl.ds((s * 48 + 8 * a) * ORDP + i, 8, stride=ORDP), :
                            ] = part[8 * a : 8 * a + 8]
            return 0

        lax.fori_loop(0, min(ORDP, ORDERS - k * ORDP) // 2, one, 0)

        def pack(n, _):
            s = n // 7
            for u in range(3):
                r = n % 7 * 3 + u
                first = stage[pl.ds(pl.multiple_of((s * 48 + r) * ORDP, 8), ORDP), :]
                second = stage[pl.ds(pl.multiple_of((s * 48 + RP + r) * ORDP, 8), ORDP), :]
                both = jnp.concatenate([first, second], axis=0).astype(jnp.bfloat16)
                f[k, s, pl.ds(pl.multiple_of(r * GROUP, 16), GROUP), :] = both
            return 0

        lax.fori_loop(0, BANDS * 7, pack, 0)

    def clear_stage(n, _):
        for i in range(ORDERS - ORDP, ORDP):
            stage[pl.ds(n * 8 * ORDP + i, 8, stride=ORDP), :] = jnp.zeros(
                (8, 128), jnp.float32
            )
        return 0

    def remote(src, dst, ss, rs, device):
        return pltpu.make_async_remote_copy(
            src_ref=src, dst_ref=dst, send_sem=ss, recv_sem=rs,
            device_id=device, device_id_type=MESH,
        )

    half = PIECEP // 2
    mine = pl.multiple_of(core * half, 16)
    other = pl.multiple_of((1 - core) * half, 16)
    in_half = pl.multiple_of(z * OWN, 16)
    own_row = pl.multiple_of(core * half + z * OWN, 16)

    def pair_sum(k):
        return remote(
            f.at[k, :, pl.ds(other, half)], buf_a.at[k], sa.at[k], ra.at[k], (c_peer, space)
        )

    def z_sums(k):
        return [
            remote(
                buf_a.at[k, :, pl.ds(pl.multiple_of((z + d) % 4 * OWN, 16), OWN)],
                buf_b.at[k, d - 1],
                sb.at[k, d - 1], rb.at[k, d - 1], (z_peers[d - 1], space),
            )
            for d in (1, 2, 3)
        ]

    def x_sum(k):
        return remote(piece.at[k], buf_c.at[k], sc.at[k], rc.at[k], (x_peer, space))

    def means_out(k):
        return [
            remote(
                buf_c.at[k, (space + d) % BANDS], mean.at[k, d, pl.ds(own_row, OWN)],
                sd.at[k, d - 1], rd.at[k, d - 1], (member, (space + d) % BANDS),
            )
            for d in range(1, BANDS)
        ]

    def z_gather(k):
        return [
            remote(
                mean.at[k, :, pl.ds(own_row, OWN)], mean.at[k, :, pl.ds(own_row, OWN)],
                sf.at[k, d - 1], rf.at[k, d - 1], (z_peers[d - 1], space),
            )
            for d in (1, 2, 3)
        ]

    def core_gather(k):
        return remote(
            mean.at[k, :, pl.ds(mine, half)], mean.at[k, :, pl.ds(mine, half)],
            sg.at[k], rg.at[k], (c_peer, space),
        )

    def raw(k, part, at, size):
        return [
            remote(
                f.at[k, (space + d) % BANDS, pl.ds(at, size)], got.at[k, d, pl.ds(at, size)],
                raw_s.at[part, d - 1], raw_r.at[part, d - 1],
                (member, (space + d) % BANDS),
            )
            for d in range(1, BANDS)
        ]

    def begin(copies):
        for copy in copies:
            copy.start()

    def finish(copies):
        for copy in copies:
            copy.wait()

    def add_pair(k):
        def one(n, _):
            s, at = n // 4, pl.multiple_of(n % 4 * OWN, 16)
            total = buf_a[k, s, pl.ds(at, OWN), :].astype(jnp.float32)
            total += f[k, s, pl.ds(mine + at, OWN), :].astype(jnp.float32)
            buf_a[k, s, pl.ds(at, OWN), :] = total.astype(jnp.bfloat16)
            return 0

        lax.fori_loop(0, BANDS * 4, one, 0)

    def add_four(k):
        def one(s, _):
            total = buf_a[k, s, pl.ds(in_half, OWN), :].astype(jnp.float32)
            for d in range(3):
                total += buf_b[k, d, s].astype(jnp.float32)
            piece[k, s] = total.astype(jnp.bfloat16)
            return 0

        lax.fori_loop(0, BANDS, one, 0)

    def add_two(k):
        def one(s, _):
            total = buf_c[k, s].astype(jnp.float32) + piece[k, s].astype(jnp.float32)
            buf_c[k, s] = (total * (1.0 / 16.0)).astype(jnp.bfloat16)
            return 0

        lax.fori_loop(0, BANDS, one, 0)
        mean[k, 0, pl.ds(own_row, OWN), :] = buf_c[k, space]

    def centre(k):
        def one(n, _):
            d, at = n // 9, pl.multiple_of(n % 9 * 112, 16)
            s = (space + BANDS - d) % BANDS
            block = got[k, d, pl.ds(at, 112), :].astype(jnp.float32)
            block = block - mean[k, d, pl.ds(at, 112), :].astype(jnp.float32)
            out_ref[s, k, pl.ds(at, 112), :] = block.astype(jnp.bfloat16)
            return 0

        def own(n, _):
            at = pl.multiple_of(n * 112, 16)
            block = f[k, space, pl.ds(at, 112), :].astype(jnp.float32)
            block = block - mean[k, 0, pl.ds(at, 112), :].astype(jnp.float32)
            out_ref[space, k, pl.ds(at, 112), :] = block.astype(jnp.bfloat16)
            return 0

        lax.fori_loop(9, BANDS * 9, one, 0)
        lax.fori_loop(0, 9, own, 0)

    column = lax.broadcasted_iota(jnp.int32, (ORDP, LON), 1).astype(jnp.float32)
    index = lax.broadcasted_iota(jnp.int32, (ORDP, LON), 0)

    def basis():
        def one(n, _):
            order = n // CHUNKS * ORDERS + n % CHUNKS * ORDP + index
            product = order.astype(jnp.float32) * column
            turns = jnp.floor((product + 0.5) * (1.0 / LON))
            angle = 2.0 * math.pi / LON * (product - turns * LON)
            weight = jnp.where(order == 0, 1.0, math.sqrt(2.0))
            weight = jnp.where(n % CHUNKS * ORDP + index < ORDERS, weight, 0.0)
            both = jnp.concatenate(
                [weight * jnp.cos(angle), weight * jnp.sin(angle)], axis=0
            )
            basis_ref[pl.ds(pl.multiple_of(n * GROUP, 16), GROUP), :] = both.astype(
                jnp.bfloat16
            )
            return 0

        lax.fori_loop(0, BANDS * CHUNKS, one, 0)

    table(0, False)
    orders_of(0)
    pl.semaphore_wait(barrier, 5 + BANDS - 1)
    a0, a1 = pair_sum(0), pair_sum(1)
    a0.start()
    raw0 = raw(0, 0, 0, PIECE)
    begin(raw0)
    lax.fori_loop(0, BANDS * 48 // 8, clear_stage, 0)
    table(1, True)
    a0.wait()
    add_pair(0)
    b0, b1 = z_sums(0), z_sums(1)
    begin(b0)
    orders_of(1)
    a1.start()
    finish(b0)
    add_four(0)
    c0, c1 = x_sum(0), x_sum(1)
    c0.start()
    a1.wait()
    add_pair(1)
    begin(b1)
    basis()
    c0.wait()
    add_two(0)
    d0, d1 = means_out(0), means_out(1)
    begin(d0)
    finish(b1)
    add_four(1)
    c1.start()
    raw1 = raw(1, 1, 0, 512)
    begin(raw1)
    finish(d0)
    f0, f1 = z_gather(0), z_gather(1)
    begin(f0)
    c1.wait()
    add_two(1)
    begin(d1)
    raw2 = raw(1, 2, 512, PIECE - 512)
    begin(raw2)
    finish(f0)
    g0, g1 = core_gather(0), core_gather(1)
    g0.start()
    finish(d1)
    begin(f1)
    finish(raw0)
    g0.wait()
    centre(0)
    finish(f1)
    g1.start()
    finish(raw1)
    finish(raw2)
    g1.wait()
    centre(1)


def fourier_blocks(coefficients, cosine, diag):
    sem = pltpu.SemaphoreType.DMA
    bf = jnp.bfloat16
    return pl.pallas_call(
        fourier_kernel,
        name="fourier_blocks",
        out_shape=[
            jax.ShapeDtypeStruct((BANDS, CHUNKS, PIECE, 128), bf),
            jax.ShapeDtypeStruct((BANDS * CHUNKS * GROUP, LON), bf),
        ],
        in_specs=[
            pl.BlockSpec(memory_space=pl.ANY),
            pl.BlockSpec(memory_space=pltpu.VMEM),
            pl.BlockSpec(memory_space=pltpu.VMEM),
        ],
        out_specs=[pl.BlockSpec(memory_space=pltpu.VMEM)] * 2,
        scratch_shapes=[
            pltpu.VMEM((CH, ORDERS, 2, LP), jnp.int32),
            pltpu.VMEM((3, ORDP * MP, 128), jnp.float32),
            pltpu.VMEM((2, ORDP * LROWS, 128), jnp.float32),
            pltpu.VMEM((BANDS * 48 * ORDP, 128), jnp.float32),
            pltpu.VMEM((CHUNKS, BANDS, PIECEP, 128), bf),
            pltpu.VMEM((CHUNKS, BANDS, PIECE, 128), bf),
            pltpu.VMEM((CHUNKS, BANDS, PIECEP, 128), bf),
            pltpu.VMEM((CHUNKS, BANDS, PIECEP // 2, 128), bf),
            pltpu.VMEM((CHUNKS, 3, BANDS, OWN, 128), bf),
            pltpu.VMEM((CHUNKS, BANDS, OWN, 128), bf),
            pltpu.VMEM((CHUNKS, BANDS, OWN, 128), bf),
            sem((3,)),
            sem((3, 7)), sem((3, 7)),
            sem((2,)), sem((2,)),
            sem((2, 3)), sem((2, 3)),
            sem((2,)), sem((2,)),
            sem((2, 7)), sem((2, 7)),
            sem((2, 3)), sem((2, 3)),
            sem((2,)), sem((2,)),
        ],
        compiler_params=pltpu.CompilerParams(
            collective_id=1, has_side_effects=True, vmem_limit_bytes=63 * 2**20
        ),
    )(coefficients, cosine, diag)


RB = 3


def synthesis_kernel(f_ref, basis_ref, scale_ref, weather_ref, out_ref):
    step = pl.program_id(0)
    rows = []
    for r in range(RB):
        x = f_ref[:, :, r].reshape(BANDS * CHUNKS * GROUP, 128)
        rows.append(x.T)
    lhs = jnp.concatenate(rows, axis=0)
    noise = jnp.dot(lhs, basis_ref[...], preferred_element_type=jnp.float32)
    for r in range(RB):
        for q in range(Q):
            scale = scale_ref[q * R + step * RB + r]
            at = (r * Q + q) * 32
            out_ref[0, q, r] = (
                weather_ref[0, q, r].astype(jnp.float32) + scale * noise[at : at + 32]
            ).astype(jnp.bfloat16)


def synthesis(fourier, basis, scale, weather):
    fourier = fourier.reshape(BANDS, CHUNKS, R, GROUP, 128)
    rows = weather.shape[2]
    weather = weather.reshape(1, Q, R, rows, LON)
    block = pl.BlockSpec((1, Q, RB, rows, LON), lambda i: (0, 0, i, 0, 0))
    out = pl.pallas_call(
        synthesis_kernel,
        name="synthesis",
        grid=(R // RB,),
        out_shape=jax.ShapeDtypeStruct(weather.shape, jnp.bfloat16),
        in_specs=[
            pl.BlockSpec((BANDS, CHUNKS, RB, GROUP, 128), lambda i: (0, 0, i, 0, 0)),
            pl.BlockSpec(basis.shape, lambda i: (0, 0)),
            pl.BlockSpec(memory_space=pltpu.SMEM),
            block,
        ],
        out_specs=block,
        compiler_params=pltpu.CompilerParams(
            dimension_semantics=("arbitrary",), vmem_limit_bytes=50 * 2**20
        ),
    )(fourier, basis, scale, weather)
    return out.reshape(1, CH, rows, LON)


def tables():
    order = lax.axis_index("space") * ORDERS + jnp.arange(CHUNKS)[:, None] * ORDP
    order = order + jnp.arange(ORDP)[None, :]
    logs = diagonal_log(BANDS * ORDERS + 2)[order]
    row_first = (LON // 2 + 1 - TCOUNT) // 2
    colatitude = (
        math.pi
        * (row_first + jnp.arange(TCOUNT, dtype=jnp.int32)).astype(jnp.float32)
        / (LON // 2)
    )
    diag = jnp.exp(
        logs[:, :, None]
        - 0.5 * math.log(4.0 * math.pi)
        + order.astype(jnp.float32)[:, :, None] * jnp.log(jnp.sin(colatitude))
    )
    return jnp.cos(colatitude)[None, :], diag


def local(weather, coefficients, channel_scale):
    cosine, diag = tables()
    centred, basis = fourier_blocks(coefficients.transpose(0, 1, 3, 2, 4), cosine, diag)
    return synthesis(centred, basis, channel_scale, weather)


def solution(mesh):
    return jax.shard_map(
        local,
        mesh=mesh,
        in_specs=(P("member", None, "space", None), P("member", None, None, "space", None), P()),
        out_specs=P("member", None, "space", None),
        check_vma=False,
    )
```

```python
import functools
import math

import jax
import jax.numpy as jnp
from jax import lax
from jax.experimental import pallas as pl
from jax.experimental.pallas import tpu as pltpu
from jax.sharding import PartitionSpec as P

MESH = pl.DeviceIdType.MESH

CH = 84
LON = 1440
TCOUNT = 256
LP = 361
BANDS = 8
ORDERS = 46
CHUNKS = 2
GO = 8
GROUPS = 6
PER = 3
Q = 4
R = CH // Q
RP = 24
MROWS = 2 * Q * RP
LROWS = 392
GR = R * 2 * GO
PIECE = PER * GR
PIECEP = 1024
OWN = 128
FACTOR = math.sqrt(3.0) * math.sqrt(4.0 * math.pi) / LP * 2.0 ** (-30)


def lane_blocks(values, lane):
    low = lane < 64

    def swap(a, b, width, mask):
        ra = pltpu.roll(a, 128 - width, 1)
        rb = pltpu.roll(b, width, 1)
        return jnp.where(mask, a, rb), jnp.where(mask, ra, b)

    v0, v1, v2, v3 = values
    a0, a2 = swap(v0, v2, 64, low)
    a1, a3 = swap(v1, v3, 64, low)
    even = (lane % 64) < 32
    b0, b1 = swap(a0, a1, 32, even)
    b2, b3 = swap(a2, a3, 32, even)
    return b0, b1, b2, b3


def fourier_kernel(
    coef_ref, out_ref, basis_out,
    coef_v, lhs_v, tab, factors, stage, basis_v, f, got, mean, buf_a, buf_b, buf_c, piece,
    load_sem, out_sem, basis_sem,
    raw_s, raw_r, sa, ra, sb, rb, sc, rc, sd, rd, sf, rf, sg, rg,
):
    member, space = lax.axis_index("member"), lax.axis_index("space")
    z, xl, core = member // 4, (member // 2) % 2, member % 2

    def member_of(z, xl, core):
        return (z * 2 + xl) * 2 + core

    def real(g):
        return min(GO, ORDERS - g * GO)

    loads = [
        pltpu.make_async_copy(
            coef_ref.at[0, :, pl.ds(g * GO, real(g))],
            coef_v.at[:, pl.ds(g * GO, real(g))],
            load_sem.at[g],
        )
        for g in range(GROUPS)
    ]
    for load in loads:
        load.start()

    z_peers = [member_of((z + d) % 4, xl, core) for d in (1, 2, 3)]
    x_peer = member_of(z, 1 - xl, core)
    c_peer = member_of(z, xl, 1 - core)
    s_peers = [(space + d) % BANDS for d in range(1, BANDS)]
    barrier = pltpu.get_barrier_semaphore()
    for peer in z_peers + [x_peer, c_peer]:
        pl.semaphore_signal(barrier, inc=1, device_id=(peer, space), device_id_type=MESH)
    for peer in s_peers:
        pl.semaphore_signal(barrier, inc=1, device_id=(member, peer), device_id_type=MESH)

    def clear_pads(n, _):
        lhs_v[2, pl.ds(pl.multiple_of(n * MROWS, 8), MROWS), :] = jnp.zeros(
            (MROWS, 128), jnp.float32
        )
        for h in range(2):
            for at in range(LP // 8 * 8, 384, 8):
                tab[h, pl.ds(pl.multiple_of(n * LROWS + at, 8), 8), :] = jnp.zeros(
                    (8, 128), jnp.float32
                )
        return 0

    lax.fori_loop(0, GO, clear_pads, 0)
    for k in range(CHUNKS):
        for s in range(BANDS):
            f[k, s, pl.ds(PIECE, PIECEP - PIECE), :] = jnp.zeros(
                (PIECEP - PIECE, 128), jnp.bfloat16
            )

    row_first = (LON // 2 + 1 - TCOUNT) // 2
    colatitude = (
        math.pi
        * (row_first + lax.broadcasted_iota(jnp.int32, (GO, TCOUNT), 1)).astype(jnp.float32)
        / (LON // 2)
    )
    cosine = jnp.cos(colatitude)
    log_sine = jnp.log(jnp.sin(colatitude))

    def arrange(g, c, i):
        base = c // R * 48 + c % R
        for t in range(3):
            wide = min(128, LP - 128 * t)
            raw = coef_v[c, g * GO + i, :, pl.ds(128 * t, wide)]
            lhs_v[t, pl.ds(i * MROWS + base, 2, stride=RP), pl.ds(0, wide)] = (
                raw.astype(jnp.float32) * FACTOR
            )

    def table(g):
        first = space * ORDERS + g * GO
        order_wide = first + lax.broadcasted_iota(jnp.int32, (GO, TCOUNT), 0)
        order = (first + lax.broadcasted_iota(jnp.int32, (GO, 128), 0)).astype(jnp.float32)
        square = order * order
        degrees = [
            (tile * 128 + lax.broadcasted_iota(jnp.int32, (GO, 128), 1)).astype(jnp.float32)
            for tile in range(3)
        ]
        logs = jnp.zeros((GO, 1), jnp.float32)
        for degree in degrees:
            at_least = jnp.maximum(degree, 1.0)
            term = 0.5 * jnp.log((2.0 * at_least + 1.0) / (2.0 * at_least))
            term = jnp.where((degree >= 1.0) & (degree <= order), term, 0.0)
            logs += jnp.sum(term, axis=1, keepdims=True)
        diag = jnp.exp(
            logs - 0.5 * math.log(4.0 * math.pi) + order_wide.astype(jnp.float32) * log_sine
        )

        def spread(tile, _):
            degree = tile * 128 + lax.broadcasted_iota(jnp.int32, (GO, 128), 1)
            degree = degree.astype(jnp.float32)
            degree_square = degree * degree
            prior = degree - 1.0
            up = jnp.sqrt(
                jnp.maximum(4.0 * degree_square - 1.0, 1.0)
                / jnp.maximum(degree_square - square, 1.0)
            )
            down = up * jnp.sqrt(
                jnp.maximum(prior * prior - square, 0.0)
                / jnp.maximum(4.0 * prior * prior - 1.0, 1.0)
            )
            for u in range(128):
                row = pl.multiple_of((tile * 128 + u) * GO, 8)
                factors[0, pl.ds(row, GO), :] = jnp.broadcast_to(up[:, u : u + 1], (GO, 128))
                factors[1, pl.ds(row, GO), :] = jnp.broadcast_to(down[:, u : u + 1], (GO, 128))
            return 0

        lax.fori_loop(0, 3, spread, 0)
        loads[g].wait()
        half_order = order_wide[:, :128]

        def block(j, carry, steps=8, channels=True):
            older, newer = carry
            for u in range(steps):
                deg = j * 8 + u
                row = pl.multiple_of(deg * GO, 8)
                up = factors[0, pl.ds(row, GO), :]
                down = factors[1, pl.ds(row, GO), :]
                here = half_order == deg
                fresh = []
                for h in range(2):
                    at = slice(128 * h, 128 * h + 128)
                    seed = jnp.where(here, diag[:, at], 0.0)
                    value = (up * cosine[:, at]) * newer[h] + (seed - down * older[h])
                    tab[h, pl.ds(deg, 8, stride=LROWS), :] = value
                    fresh.append(value)
                older, newer = newer, tuple(fresh)
                if channels:
                    for i in (u % 4 * 2, u % 4 * 2 + 1):
                        if i < real(g):
                            arrange(g, j * 2 + u // 4, i)
            return older, newer

        zero = jnp.zeros((GO, 128), jnp.float32)
        carry = ((zero, zero), (zero, zero))
        carry = lax.fori_loop(0, CH // 2, block, carry)
        carry = lax.fori_loop(
            CH // 2, LP // 8, functools.partial(block, channels=False), carry
        )
        block(LP // 8, carry, steps=LP % 8, channels=False)

    lane = lax.broadcasted_iota(jnp.int32, (RP * 2, 128), 1)

    def orders_of(g):
        k, at_group = g // PER, g % PER * GR

        def one(n, _):
            for i in (2 * n, 2 * n + 1):
                row = pl.multiple_of(i * MROWS, 8)
                lhs = jnp.concatenate(
                    [lhs_v[t, pl.ds(row, MROWS), :].astype(jnp.bfloat16) for t in range(3)],
                    axis=1,
                )
                row = pl.multiple_of(i * LROWS, 8)
                rhs = jnp.concatenate(
                    [tab[h, pl.ds(row, 384), :].astype(jnp.bfloat16) for h in range(2)], axis=1
                )
                out = jnp.dot(lhs, rhs, preferred_element_type=jnp.float32)
                for h in range(2):
                    parts = [
                        out[48 * q : 48 * q + 48, 128 * h : 128 * h + 128] for q in range(Q)
                    ]
                    for b, part in enumerate(lane_blocks(parts, lane)):
                        s = 4 * h + b
                        for a in range(6):
                            stage[pl.ds((s * 48 + 8 * a) * GO + i, 8, stride=GO), :] = part[
                                8 * a : 8 * a + 8
                            ]
            return 0

        if real(g) < GO:

            def clear_stage(n, _):
                for i in range(real(g), GO):
                    stage[pl.ds(n * 8 * GO + i, 8, stride=GO), :] = jnp.zeros(
                        (8, 128), jnp.float32
                    )
                return 0

            lax.fori_loop(0, BANDS * 48 // 8, clear_stage, 0)
        lax.fori_loop(0, real(g) // 2, one, 0)

        def pack(n, _):
            s = n // 3
            for u in range(7):
                r = n % 3 * 7 + u
                first = stage[pl.ds(pl.multiple_of((s * 48 + r) * GO, 8), GO), :]
                second = stage[pl.ds(pl.multiple_of((s * 48 + RP + r) * GO, 8), GO), :]
                both = jnp.concatenate([first, second], axis=0).astype(jnp.bfloat16)
                f[k, s, pl.ds(pl.multiple_of(at_group + r * 2 * GO, 16), 2 * GO), :] = both
            return 0

        lax.fori_loop(0, BANDS * 3, pack, 0)

    def remote(src, dst, ss, rs, device):
        return pltpu.make_async_remote_copy(
            src_ref=src, dst_ref=dst, send_sem=ss, recv_sem=rs,
            device_id=device, device_id_type=MESH,
        )

    half = PIECEP // 2
    mine = pl.multiple_of(core * half, 16)
    other = pl.multiple_of((1 - core) * half, 16)
    in_half = pl.multiple_of(z * OWN, 16)
    own_row = pl.multiple_of(core * half + z * OWN, 16)

    def pair_sum(k):
        return remote(
            f.at[k, :, pl.ds(other, half)], buf_a.at[k], sa.at[k], ra.at[k], (c_peer, space)
        )

    def z_sums(k):
        return [
            remote(
                buf_a.at[k, :, pl.ds(pl.multiple_of((z + d) % 4 * OWN, 16), OWN)],
                buf_b.at[k, d - 1],
                sb.at[k, d - 1], rb.at[k, d - 1], (z_peers[d - 1], space),
            )
            for d in (1, 2, 3)
        ]

    def x_sum(k):
        return remote(piece.at[k], buf_c.at[k], sc.at[k], rc.at[k], (x_peer, space))

    def means_out(k):
        return [
            remote(
                buf_c.at[k, (space + d) % BANDS], mean.at[k, d, pl.ds(own_row, OWN)],
                sd.at[k, d - 1], rd.at[k, d - 1], (member, (space + d) % BANDS),
            )
            for d in range(1, BANDS)
        ]

    def z_gather(k):
        return [
            remote(
                mean.at[k, :, pl.ds(own_row, OWN)], mean.at[k, :, pl.ds(own_row, OWN)],
                sf.at[k, d - 1], rf.at[k, d - 1], (z_peers[d - 1], space),
            )
            for d in (1, 2, 3)
        ]

    def core_gather(k):
        return remote(
            mean.at[k, :, pl.ds(mine, half)], mean.at[k, :, pl.ds(mine, half)],
            sg.at[k], rg.at[k], (c_peer, space),
        )

    def raw(k, part, at, size):
        return [
            remote(
                f.at[k, (space + d) % BANDS, pl.ds(at, size)], got.at[k, d, pl.ds(at, size)],
                raw_s.at[part, d - 1], raw_r.at[part, d - 1],
                (member, (space + d) % BANDS),
            )
            for d in range(1, BANDS)
        ]

    def begin(copies):
        for copy in copies:
            copy.start()

    def finish(copies):
        for copy in copies:
            copy.wait()

    def add_pair(k):
        def one(n, _):
            s, at = n // 4, pl.multiple_of(n % 4 * OWN, 16)
            total = buf_a[k, s, pl.ds(at, OWN), :].astype(jnp.float32)
            total += f[k, s, pl.ds(mine + at, OWN), :].astype(jnp.float32)
            buf_a[k, s, pl.ds(at, OWN), :] = total.astype(jnp.bfloat16)
            return 0

        lax.fori_loop(0, BANDS * 4, one, 0)

    def add_four(k):
        def one(s, _):
            total = buf_a[k, s, pl.ds(in_half, OWN), :].astype(jnp.float32)
            for d in range(3):
                total += buf_b[k, d, s].astype(jnp.float32)
            piece[k, s] = total.astype(jnp.bfloat16)
            return 0

        lax.fori_loop(0, BANDS, one, 0)

    def add_two(k):
        def one(s, _):
            total = buf_c[k, s].astype(jnp.float32) + piece[k, s].astype(jnp.float32)
            buf_c[k, s] = (total * (1.0 / 16.0)).astype(jnp.bfloat16)
            return 0

        lax.fori_loop(0, BANDS, one, 0)
        mean[k, 0, pl.ds(own_row, OWN), :] = buf_c[k, space]

    def outs(k, d):
        return pltpu.make_async_copy(
            got.at[k, d], out_ref.at[(space + BANDS - d) % BANDS, k], out_sem.at[k, d]
        )

    def centre(k):
        for d in range(BANDS):

            def one(n, _):
                at = pl.multiple_of(n * 112, 16)
                block = f[k, space, pl.ds(at, 112), :] if d == 0 else got[k, d, pl.ds(at, 112), :]
                block = block.astype(jnp.float32) - mean[k, d, pl.ds(at, 112), :].astype(
                    jnp.float32
                )
                got[k, d, pl.ds(at, 112), :] = block.astype(jnp.bfloat16)
                return 0

            lax.fori_loop(0, 9, one, 0)
            outs(k, d).start()

    column = lax.broadcasted_iota(jnp.int32, (GO, LON), 1).astype(jnp.float32)
    index = lax.broadcasted_iota(jnp.int32, (GO, LON), 0)

    def basis():
        def one(n, _):
            slot = n % GROUPS * GO + index
            order = n // GROUPS * ORDERS + slot
            product = order.astype(jnp.float32) * column
            turns = jnp.floor((product + 0.5) * (1.0 / LON))
            angle = 2.0 * math.pi / LON * (product - turns * LON)
            weight = jnp.where(order == 0, 1.0, math.sqrt(2.0))
            weight = jnp.where(slot < ORDERS, weight, 0.0)
            both = jnp.concatenate(
                [weight * jnp.cos(angle), weight * jnp.sin(angle)], axis=0
            )
            basis_v[pl.ds(pl.multiple_of(n * 2 * GO, 16), 2 * GO), :] = both.astype(
                jnp.bfloat16
            )
            return 0

        lax.fori_loop(0, BANDS * GROUPS, one, 0)

    def group(g):
        table(g)
        orders_of(g)

    def raw_group(part, g, at=0, size=GR):
        return raw(g // PER, part, g % PER * GR + at, size)

    a0, a1 = pair_sum(0), pair_sum(1)
    b0, b1 = z_sums(0), z_sums(1)
    c0, c1 = x_sum(0), x_sum(1)
    d0, d1 = means_out(0), means_out(1)
    f0, f1 = z_gather(0), z_gather(1)
    g0, g1 = core_gather(0), core_gather(1)
    raws = [
        raw_group(0, 0),
        raw_group(1, 1),
        raw_group(2, 2),
        raw_group(3, 3, 0, 176),
        raw_group(4, 3, 176, GR - 176),
        raw_group(5, 4),
        raw_group(6, 5),
    ]

    group(0)
    pl.semaphore_wait(barrier, 5 + BANDS - 1)
    begin(raws[0])
    group(1)
    begin(raws[1])
    group(2)
    a0.start()
    begin(raws[2])
    table(3)
    a0.wait()
    add_pair(0)
    begin(b0)
    orders_of(3)
    begin(raws[3])
    group(4)
    group(5)
    a1.start()
    finish(b0)
    add_four(0)
    c0.start()
    a1.wait()
    add_pair(1)
    begin(b1)
    basis()
    basis_copy = pltpu.make_async_copy(basis_v, basis_out, basis_sem)
    basis_copy.start()
    c0.wait()
    add_two(0)
    begin(d0)
    begin(raws[4])
    finish(d0)
    begin(f0)
    finish(b1)
    add_four(1)
    c1.start()
    c1.wait()
    add_two(1)
    begin(d1)
    begin(raws[5])
    begin(raws[6])
    finish(f0)
    g0.start()
    finish(d1)
    begin(f1)
    finish(raws[0])
    finish(raws[1])
    finish(raws[2])
    g0.wait()
    centre(0)
    finish(f1)
    g1.start()
    for copies in raws[3:]:
        finish(copies)
    g1.wait()
    centre(1)
    basis_copy.wait()
    for k in range(CHUNKS):
        for d in range(BANDS):
            outs(k, d).wait()


def fourier_blocks(coefficients):
    sem = pltpu.SemaphoreType.DMA
    bf = jnp.bfloat16
    basis = (BANDS * GROUPS * 2 * GO, LON)
    return pl.pallas_call(
        fourier_kernel,
        name="fourier_blocks",
        out_shape=[
            jax.ShapeDtypeStruct((BANDS, CHUNKS, PIECE, 128), bf),
            jax.ShapeDtypeStruct(basis, bf),
        ],
        in_specs=[pl.BlockSpec(memory_space=pl.ANY)],
        out_specs=[pl.BlockSpec(memory_space=pl.ANY)] * 2,
        scratch_shapes=[
            pltpu.VMEM((CH, ORDERS, 2, LP), jnp.int32),
            pltpu.VMEM((3, GO * MROWS, 128), jnp.float32),
            pltpu.VMEM((2, GO * LROWS, 128), jnp.float32),
            pltpu.VMEM((2, 384 * GO, 128), jnp.float32),
            pltpu.VMEM((BANDS * 48 * GO, 128), jnp.float32),
            pltpu.VMEM(basis, bf),
            pltpu.VMEM((CHUNKS, BANDS, PIECEP, 128), bf),
            pltpu.VMEM((CHUNKS, BANDS, PIECE, 128), bf),
            pltpu.VMEM((CHUNKS, BANDS, PIECEP, 128), bf),
            pltpu.VMEM((CHUNKS, BANDS, PIECEP // 2, 128), bf),
            pltpu.VMEM((CHUNKS, 3, BANDS, OWN, 128), bf),
            pltpu.VMEM((CHUNKS, BANDS, OWN, 128), bf),
            pltpu.VMEM((CHUNKS, BANDS, OWN, 128), bf),
            sem((GROUPS,)), sem((CHUNKS, BANDS)), sem,
            sem((7, 7)), sem((7, 7)),
            sem((2,)), sem((2,)),
            sem((2, 3)), sem((2, 3)),
            sem((2,)), sem((2,)),
            sem((2, 7)), sem((2, 7)),
            sem((2, 3)), sem((2, 3)),
            sem((2,)), sem((2,)),
        ],
        compiler_params=pltpu.CompilerParams(
            collective_id=1, has_side_effects=True, vmem_limit_bytes=63 * 2**20
        ),
    )(coefficients)


RB = 3


def synthesis_kernel(f_ref, basis_ref, scale_ref, weather_ref, out_ref):
    step = pl.program_id(0)
    rows = []
    for r in range(RB):
        x = f_ref[:, :, r].reshape(BANDS * GROUPS * 2 * GO, 128)
        rows.append(x.T)
    lhs = jnp.concatenate(rows, axis=0)
    noise = jnp.dot(lhs, basis_ref[...], preferred_element_type=jnp.float32)
    for r in range(RB):
        for q in range(Q):
            scale = scale_ref[q * R + step * RB + r]
            at = (r * Q + q) * 32
            out_ref[0, q, r] = (
                weather_ref[0, q, r].astype(jnp.float32) + scale * noise[at : at + 32]
            ).astype(jnp.bfloat16)


def synthesis(fourier, basis, scale, weather):
    fourier = fourier.reshape(BANDS, GROUPS, R, 2 * GO, 128)
    rows = weather.shape[2]
    weather = weather.reshape(1, Q, R, rows, LON)
    block = pl.BlockSpec((1, Q, RB, rows, LON), lambda i: (0, 0, i, 0, 0))
    out = pl.pallas_call(
        synthesis_kernel,
        name="synthesis",
        grid=(R // RB,),
        out_shape=jax.ShapeDtypeStruct(weather.shape, jnp.bfloat16),
        in_specs=[
            pl.BlockSpec((BANDS, GROUPS, RB, 2 * GO, 128), lambda i: (0, 0, i, 0, 0)),
            pl.BlockSpec(basis.shape, lambda i: (0, 0)),
            pl.BlockSpec(memory_space=pltpu.SMEM),
            block,
        ],
        out_specs=block,
        compiler_params=pltpu.CompilerParams(
            dimension_semantics=("arbitrary",), vmem_limit_bytes=63 * 2**20
        ),
    )(fourier, basis, scale, weather)
    return out.reshape(1, CH, rows, LON)


def local(weather, coefficients, channel_scale):
    centred, basis = fourier_blocks(coefficients.transpose(0, 1, 3, 2, 4))
    return synthesis(centred, basis, channel_scale, weather)


def solution(mesh):
    return jax.shard_map(
        local,
        mesh=mesh,
        in_specs=(P("member", None, "space", None), P("member", None, None, "space", None), P()),
        out_specs=P("member", None, "space", None),
        check_vma=False,
    )
```

```python
import functools
import math

import jax
import jax.numpy as jnp
from jax import lax
from jax.experimental import pallas as pl
from jax.experimental.pallas import tpu as pltpu
from jax.sharding import PartitionSpec as P

MESH = pl.DeviceIdType.MESH

CH = 84
LON = 1440
TCOUNT = 256
LP = 361
BANDS = 8
ORDERS = 46
CHUNKS = 2
GO = 8
GROUPS = 6
PER = 3
Q = 4
R = CH // Q
RP = 24
MROWS = 2 * Q * RP
LROWS = 392
GR = R * 2 * GO
PIECE = PER * GR
PIECEP = 1024
OWN = 128
FACTOR = math.sqrt(3.0) * math.sqrt(4.0 * math.pi) / LP * 2.0 ** (-30)


def lane_blocks(values, lane):
    low = lane < 64

    def swap(a, b, width, mask):
        ra = pltpu.roll(a, 128 - width, 1)
        rb = pltpu.roll(b, width, 1)
        return jnp.where(mask, a, rb), jnp.where(mask, ra, b)

    v0, v1, v2, v3 = values
    a0, a2 = swap(v0, v2, 64, low)
    a1, a3 = swap(v1, v3, 64, low)
    even = (lane % 64) < 32
    b0, b1 = swap(a0, a1, 32, even)
    b2, b3 = swap(a2, a3, 32, even)
    return b0, b1, b2, b3


def fourier_kernel(
    coef_ref, out_ref, basis_out,
    coef_v, lhs_v, tab, factors, stage, basis_v, f, got, mean, buf_a, buf_b, buf_c, piece,
    load_sem, out_sem, basis_sem,
    raw_s, raw_r, sa, ra, sb, rb, sc, rc, sd, rd, sf, rf, sg, rg,
):
    member, space = lax.axis_index("member"), lax.axis_index("space")
    z, xl, core = member // 4, (member // 2) % 2, member % 2

    def member_of(z, xl, core):
        return (z * 2 + xl) * 2 + core

    def real(g):
        return min(GO, ORDERS - g * GO)

    loads = [
        pltpu.make_async_copy(
            coef_ref.at[0, :, pl.ds(g * GO, real(g))],
            coef_v.at[:, pl.ds(g * GO, real(g))],
            load_sem.at[g],
        )
        for g in range(GROUPS)
    ]
    for load in loads:
        load.start()

    z_peers = [member_of((z + d) % 4, xl, core) for d in (1, 2, 3)]
    x_peer = member_of(z, 1 - xl, core)
    c_peer = member_of(z, xl, 1 - core)
    s_peers = [(space + d) % BANDS for d in range(1, BANDS)]
    barrier = pltpu.get_barrier_semaphore()
    for peer in z_peers + [x_peer, c_peer]:
        pl.semaphore_signal(barrier, inc=1, device_id=(peer, space), device_id_type=MESH)
    for peer in s_peers:
        pl.semaphore_signal(barrier, inc=1, device_id=(member, peer), device_id_type=MESH)

    def clear_pads(n, _):
        lhs_v[2, pl.ds(pl.multiple_of(n * MROWS, 8), MROWS), :] = jnp.zeros(
            (MROWS, 128), jnp.float32
        )
        for h in range(2):
            for at in range(LP // 8 * 8, 384, 8):
                tab[h, pl.ds(pl.multiple_of(n * LROWS + at, 8), 8), :] = jnp.zeros(
                    (8, 128), jnp.float32
                )
        return 0

    lax.fori_loop(0, GO, clear_pads, 0)
    for k in range(CHUNKS):
        for s in range(BANDS):
            f[k, s, pl.ds(PIECE, PIECEP - PIECE), :] = jnp.zeros(
                (PIECEP - PIECE, 128), jnp.bfloat16
            )

    row_first = (LON // 2 + 1 - TCOUNT) // 2
    colatitude = (
        math.pi
        * (row_first + lax.broadcasted_iota(jnp.int32, (GO, TCOUNT), 1)).astype(jnp.float32)
        / (LON // 2)
    )
    cosine = jnp.cos(colatitude)
    log_sine = jnp.log(jnp.sin(colatitude))

    def arrange(g, c, i):
        base = c // R * 48 + c % R
        for t in range(3):
            wide = min(128, LP - 128 * t)
            raw = coef_v[c, g * GO + i, :, pl.ds(128 * t, wide)]
            lhs_v[t, pl.ds(i * MROWS + base, 2, stride=RP), pl.ds(0, wide)] = (
                raw.astype(jnp.float32) * FACTOR
            )

    def table(g):
        first = space * ORDERS + g * GO
        order_wide = first + lax.broadcasted_iota(jnp.int32, (GO, TCOUNT), 0)
        order = (first + lax.broadcasted_iota(jnp.int32, (GO, 128), 0)).astype(jnp.float32)
        square = order * order
        degrees = [
            (tile * 128 + lax.broadcasted_iota(jnp.int32, (GO, 128), 1)).astype(jnp.float32)
            for tile in range(3)
        ]
        logs = jnp.zeros((GO, 1), jnp.float32)
        for degree in degrees:
            at_least = jnp.maximum(degree, 1.0)
            term = 0.5 * jnp.log((2.0 * at_least + 1.0) / (2.0 * at_least))
            term = jnp.where((degree >= 1.0) & (degree <= order), term, 0.0)
            logs += jnp.sum(term, axis=1, keepdims=True)
        diag = jnp.exp(
            logs - 0.5 * math.log(4.0 * math.pi) + order_wide.astype(jnp.float32) * log_sine
        )

        def spread(tile, _):
            degree = tile * 128 + lax.broadcasted_iota(jnp.int32, (GO, 128), 1)
            degree = degree.astype(jnp.float32)
            degree_square = degree * degree
            up = jnp.sqrt(
                jnp.maximum(4.0 * degree_square - 1.0, 1.0)
                / jnp.maximum(degree_square - square, 1.0)
            )
            for u in range(128):
                row = pl.multiple_of((tile * 128 + u) * GO, 8)
                factors[pl.ds(row, GO), :] = jnp.broadcast_to(up[:, u : u + 1], (GO, 128))
            return 0

        lax.fori_loop(0, 3, spread, 0)
        loads[g].wait()
        half_order = order_wide[:, :128]

        def block(j, carry, steps=8, channels=True):
            older, newer, down = carry
            for u in range(steps):
                deg = j * 8 + u
                row = pl.multiple_of(deg * GO, 8)
                up = factors[pl.ds(row, GO), :]
                both = up * down
                here = half_order == deg
                fresh = []
                for h in range(2):
                    at = slice(128 * h, 128 * h + 128)
                    seed = jnp.where(here, diag[:, at], 0.0)
                    value = (up * cosine[:, at]) * newer[h] + (seed - both * older[h])
                    tab[h, pl.ds(deg, 8, stride=LROWS), :] = value
                    fresh.append(value)
                older, newer, down = newer, tuple(fresh), 1.0 / up
                if channels:
                    for i in (u % 4 * 2, u % 4 * 2 + 1):
                        if i < real(g):
                            arrange(g, j * 2 + u // 4, i)
            return older, newer, down

        zero = jnp.zeros((GO, 128), jnp.float32)
        carry = ((zero, zero), (zero, zero), zero)
        carry = lax.fori_loop(0, CH // 2, block, carry)
        carry = lax.fori_loop(
            CH // 2, LP // 8, functools.partial(block, channels=False), carry
        )
        block(LP // 8, carry, steps=LP % 8, channels=False)

    lane = lax.broadcasted_iota(jnp.int32, (RP * 2, 128), 1)

    def orders_of(g):
        k, at_group = g // PER, g % PER * GR

        def one(n, _):
            for i in (2 * n, 2 * n + 1):
                row = pl.multiple_of(i * MROWS, 8)
                lhs = jnp.concatenate(
                    [lhs_v[t, pl.ds(row, MROWS), :].astype(jnp.bfloat16) for t in range(3)],
                    axis=1,
                )
                row = pl.multiple_of(i * LROWS, 8)
                rhs = jnp.concatenate(
                    [tab[h, pl.ds(row, 384), :].astype(jnp.bfloat16) for h in range(2)], axis=1
                )
                out = jnp.dot(lhs, rhs, preferred_element_type=jnp.float32)
                for h in range(2):
                    parts = [
                        out[48 * q : 48 * q + 48, 128 * h : 128 * h + 128] for q in range(Q)
                    ]
                    for b, part in enumerate(lane_blocks(parts, lane)):
                        s = 4 * h + b
                        for a in range(6):
                            stage[pl.ds((s * 48 + 8 * a) * GO + i, 8, stride=GO), :] = part[
                                8 * a : 8 * a + 8
                            ]
            return 0

        if real(g) < GO:

            def clear_stage(n, _):
                for i in range(real(g), GO):
                    stage[pl.ds(n * 8 * GO + i, 8, stride=GO), :] = jnp.zeros(
                        (8, 128), jnp.float32
                    )
                return 0

            lax.fori_loop(0, BANDS * 48 // 8, clear_stage, 0)
        lax.fori_loop(0, real(g) // 2, one, 0)

        def pack(n, _):
            s = n // 3
            for u in range(7):
                r = n % 3 * 7 + u
                first = stage[pl.ds(pl.multiple_of((s * 48 + r) * GO, 8), GO), :]
                second = stage[pl.ds(pl.multiple_of((s * 48 + RP + r) * GO, 8), GO), :]
                both = jnp.concatenate([first, second], axis=0).astype(jnp.bfloat16)
                f[k, s, pl.ds(pl.multiple_of(at_group + r * 2 * GO, 16), 2 * GO), :] = both
            return 0

        lax.fori_loop(0, BANDS * 3, pack, 0)

    def remote(src, dst, ss, rs, device):
        return pltpu.make_async_remote_copy(
            src_ref=src, dst_ref=dst, send_sem=ss, recv_sem=rs,
            device_id=device, device_id_type=MESH,
        )

    half = PIECEP // 2
    mine = pl.multiple_of(core * half, 16)
    other = pl.multiple_of((1 - core) * half, 16)
    in_half = pl.multiple_of(z * OWN, 16)
    own_row = pl.multiple_of(core * half + z * OWN, 16)

    def pair_sum(k):
        return remote(
            f.at[k, :, pl.ds(other, half)], buf_a.at[k], sa.at[k], ra.at[k], (c_peer, space)
        )

    def z_sums(k):
        return [
            remote(
                buf_a.at[k, :, pl.ds(pl.multiple_of((z + d) % 4 * OWN, 16), OWN)],
                buf_b.at[k, d - 1],
                sb.at[k, d - 1], rb.at[k, d - 1], (z_peers[d - 1], space),
            )
            for d in (1, 2, 3)
        ]

    def x_sum(k):
        return remote(piece.at[k], buf_c.at[k], sc.at[k], rc.at[k], (x_peer, space))

    def means_out(k):
        return [
            remote(
                buf_c.at[k, (space + d) % BANDS], mean.at[k, d, pl.ds(own_row, OWN)],
                sd.at[k, d - 1], rd.at[k, d - 1], (member, (space + d) % BANDS),
            )
            for d in range(1, BANDS)
        ]

    def z_gather(k):
        return [
            remote(
                mean.at[k, :, pl.ds(own_row, OWN)], mean.at[k, :, pl.ds(own_row, OWN)],
                sf.at[k, d - 1], rf.at[k, d - 1], (z_peers[d - 1], space),
            )
            for d in (1, 2, 3)
        ]

    def core_gather(k):
        return remote(
            mean.at[k, :, pl.ds(mine, half)], mean.at[k, :, pl.ds(mine, half)],
            sg.at[k], rg.at[k], (c_peer, space),
        )

    def raw(k, part, at, size):
        return [
            remote(
                f.at[k, (space + d) % BANDS, pl.ds(at, size)], got.at[k, d, pl.ds(at, size)],
                raw_s.at[part, d - 1], raw_r.at[part, d - 1],
                (member, (space + d) % BANDS),
            )
            for d in range(1, BANDS)
        ]

    def begin(copies):
        for copy in copies:
            copy.start()

    def finish(copies):
        for copy in copies:
            copy.wait()

    def add_pair(k):
        def one(n, _):
            s, at = n // 4, pl.multiple_of(n % 4 * OWN, 16)
            total = buf_a[k, s, pl.ds(at, OWN), :].astype(jnp.float32)
            total += f[k, s, pl.ds(mine + at, OWN), :].astype(jnp.float32)
            buf_a[k, s, pl.ds(at, OWN), :] = total.astype(jnp.bfloat16)
            return 0

        lax.fori_loop(0, BANDS * 4, one, 0)

    def add_four(k):
        def one(s, _):
            total = buf_a[k, s, pl.ds(in_half, OWN), :].astype(jnp.float32)
            for d in range(3):
                total += buf_b[k, d, s].astype(jnp.float32)
            piece[k, s] = total.astype(jnp.bfloat16)
            return 0

        lax.fori_loop(0, BANDS, one, 0)

    def add_two(k):
        def one(s, _):
            total = buf_c[k, s].astype(jnp.float32) + piece[k, s].astype(jnp.float32)
            buf_c[k, s] = (total * (1.0 / 16.0)).astype(jnp.bfloat16)
            return 0

        lax.fori_loop(0, BANDS, one, 0)
        mean[k, 0, pl.ds(own_row, OWN), :] = buf_c[k, space]

    def outs(k, d):
        return pltpu.make_async_copy(
            got.at[k, d], out_ref.at[(space + BANDS - d) % BANDS, k], out_sem.at[k, d]
        )

    def centre(k):
        for d in range(BANDS):

            def one(n, _):
                at = pl.multiple_of(n * 112, 16)
                block = f[k, space, pl.ds(at, 112), :] if d == 0 else got[k, d, pl.ds(at, 112), :]
                block = block.astype(jnp.float32) - mean[k, d, pl.ds(at, 112), :].astype(
                    jnp.float32
                )
                got[k, d, pl.ds(at, 112), :] = block.astype(jnp.bfloat16)
                return 0

            lax.fori_loop(0, 9, one, 0)
            outs(k, d).start()

    column = lax.broadcasted_iota(jnp.int32, (GO, LON), 1).astype(jnp.float32)
    index = lax.broadcasted_iota(jnp.int32, (GO, LON), 0)

    def basis():
        def one(n, _):
            slot = n % GROUPS * GO + index
            order = n // GROUPS * ORDERS + slot
            product = order.astype(jnp.float32) * column
            turns = jnp.floor((product + 0.5) * (1.0 / LON))
            angle = 2.0 * math.pi / LON * (product - turns * LON)
            weight = jnp.where(order == 0, 1.0, math.sqrt(2.0))
            weight = jnp.where(slot < ORDERS, weight, 0.0)
            both = jnp.concatenate(
                [weight * jnp.cos(angle), weight * jnp.sin(angle)], axis=0
            )
            basis_v[pl.ds(pl.multiple_of(n * 2 * GO, 16), 2 * GO), :] = both.astype(
                jnp.bfloat16
            )
            return 0

        lax.fori_loop(0, BANDS * GROUPS, one, 0)

    def group(g):
        table(g)
        orders_of(g)

    def raw_group(part, g, at=0, size=GR):
        return raw(g // PER, part, g % PER * GR + at, size)

    a0, a1 = pair_sum(0), pair_sum(1)
    b0, b1 = z_sums(0), z_sums(1)
    c0, c1 = x_sum(0), x_sum(1)
    d0, d1 = means_out(0), means_out(1)
    f0, f1 = z_gather(0), z_gather(1)
    g0, g1 = core_gather(0), core_gather(1)
    pieces = (
        (0, 0, GR), (1, 0, GR), (2, 0, GR), (3, 0, 224),
        (3, 224, 64), (3, 288, 48), (4, 0, 64), (4, 64, 64), (4, 128, GR - 128), (5, 0, GR),
    )
    raws = [raw_group(n, *piece) for n, piece in enumerate(pieces)]

    group(0)
    pl.semaphore_wait(barrier, 5 + BANDS - 1)
    begin(raws[0])
    group(1)
    begin(raws[1])
    group(2)
    a0.start()
    begin(raws[2])
    table(3)
    a0.wait()
    add_pair(0)
    begin(b0)
    orders_of(3)
    begin(raws[3])
    group(4)
    group(5)
    a1.start()
    finish(b0)
    add_four(0)
    c0.start()
    begin(raws[4])
    a1.wait()
    add_pair(1)
    begin(b1)
    c0.wait()
    add_two(0)
    begin(d0)
    begin(raws[5])
    begin(raws[6])
    finish(d0)
    begin(f0)
    finish(b1)
    add_four(1)
    c1.start()
    begin(raws[7])
    c1.wait()
    add_two(1)
    begin(d1)
    begin(raws[8])
    begin(raws[9])
    finish(f0)
    g0.start()
    finish(d1)
    begin(f1)
    basis()
    basis_copy = pltpu.make_async_copy(basis_v, basis_out, basis_sem)
    basis_copy.start()
    finish(raws[0])
    finish(raws[1])
    finish(raws[2])
    g0.wait()
    centre(0)
    finish(f1)
    g1.start()
    for copies in raws[3:]:
        finish(copies)
    g1.wait()
    centre(1)
    basis_copy.wait()
    for k in range(CHUNKS):
        for d in range(BANDS):
            outs(k, d).wait()


def fourier_blocks(coefficients):
    sem = pltpu.SemaphoreType.DMA
    bf = jnp.bfloat16
    basis = (BANDS * GROUPS * 2 * GO, LON)
    return pl.pallas_call(
        fourier_kernel,
        name="fourier_blocks",
        out_shape=[
            jax.ShapeDtypeStruct((BANDS, CHUNKS, PIECE, 128), bf),
            jax.ShapeDtypeStruct(basis, bf),
        ],
        in_specs=[pl.BlockSpec(memory_space=pl.ANY)],
        out_specs=[pl.BlockSpec(memory_space=pl.ANY)] * 2,
        scratch_shapes=[
            pltpu.VMEM((CH, ORDERS, 2, LP), jnp.int32),
            pltpu.VMEM((3, GO * MROWS, 128), jnp.float32),
            pltpu.VMEM((2, GO * LROWS, 128), jnp.float32),
            pltpu.VMEM((384 * GO, 128), jnp.float32),
            pltpu.VMEM((BANDS * 48 * GO, 128), jnp.float32),
            pltpu.VMEM(basis, bf),
            pltpu.VMEM((CHUNKS, BANDS, PIECEP, 128), bf),
            pltpu.VMEM((CHUNKS, BANDS, PIECE, 128), bf),
            pltpu.VMEM((CHUNKS, BANDS, PIECEP, 128), bf),
            pltpu.VMEM((CHUNKS, BANDS, PIECEP // 2, 128), bf),
            pltpu.VMEM((CHUNKS, 3, BANDS, OWN, 128), bf),
            pltpu.VMEM((CHUNKS, BANDS, OWN, 128), bf),
            pltpu.VMEM((CHUNKS, BANDS, OWN, 128), bf),
            sem((GROUPS,)), sem((CHUNKS, BANDS)), sem,
            sem((10, 7)), sem((10, 7)),
            sem((2,)), sem((2,)),
            sem((2, 3)), sem((2, 3)),
            sem((2,)), sem((2,)),
            sem((2, 7)), sem((2, 7)),
            sem((2, 3)), sem((2, 3)),
            sem((2,)), sem((2,)),
        ],
        compiler_params=pltpu.CompilerParams(
            collective_id=1, has_side_effects=True, vmem_limit_bytes=63 * 2**20
        ),
    )(coefficients)


RB = 7


def synthesis_kernel(f_ref, basis_ref, scale_ref, weather_ref, out_ref):
    step = pl.program_id(0)
    rows = []
    for r in range(RB):
        x = f_ref[:, :, r].reshape(BANDS * GROUPS * 2 * GO, 128)
        rows.append(x.T)
    lhs = jnp.concatenate(rows, axis=0)
    noise = jnp.dot(lhs, basis_ref[...], preferred_element_type=jnp.float32)
    for r in range(RB):
        for q in range(Q):
            scale = scale_ref[q * R + step * RB + r]
            at = (r * Q + q) * 32
            out_ref[0, q, r] = (
                weather_ref[0, q, r].astype(jnp.float32) + scale * noise[at : at + 32]
            ).astype(jnp.bfloat16)


def synthesis(fourier, basis, scale, weather):
    fourier = fourier.reshape(BANDS, GROUPS, R, 2 * GO, 128)
    rows = weather.shape[2]
    weather = weather.reshape(1, Q, R, rows, LON)
    block = pl.BlockSpec((1, Q, RB, rows, LON), lambda i: (0, 0, i, 0, 0))
    out = pl.pallas_call(
        synthesis_kernel,
        name="synthesis",
        grid=(R // RB,),
        out_shape=jax.ShapeDtypeStruct(weather.shape, jnp.bfloat16),
        in_specs=[
            pl.BlockSpec((BANDS, GROUPS, RB, 2 * GO, 128), lambda i: (0, 0, i, 0, 0)),
            pl.BlockSpec(basis.shape, lambda i: (0, 0)),
            pl.BlockSpec(memory_space=pltpu.SMEM),
            block,
        ],
        out_specs=block,
        compiler_params=pltpu.CompilerParams(
            dimension_semantics=("arbitrary",), vmem_limit_bytes=63 * 2**20
        ),
    )(fourier, basis, scale, weather)
    return out.reshape(1, CH, rows, LON)


def local(weather, coefficients, channel_scale):
    centred, basis = fourier_blocks(coefficients.transpose(0, 1, 3, 2, 4))
    return synthesis(centred, basis, channel_scale, weather)


def solution(mesh):
    return jax.shard_map(
        local,
        mesh=mesh,
        in_specs=(P("member", None, "space", None), P("member", None, None, "space", None), P()),
        out_specs=P("member", None, "space", None),
        check_vma=False,
    )
```

```python
import functools
import math

import jax
import jax.numpy as jnp
from jax import lax
from jax.experimental import pallas as pl
from jax.experimental.pallas import tpu as pltpu
from jax.sharding import PartitionSpec as P

MESH = pl.DeviceIdType.MESH

CH = 84
LON = 1440
TCOUNT = 256
LP = 361
BANDS = 8
ORDERS = 46
CHUNKS = 2
GO = 8
GROUPS = 6
PER = 3
Q = 4
R = CH // Q
RP = 24
MROWS = 2 * Q * RP
LROWS = 392
GR = R * 2 * GO
PIECE = PER * GR
PIECEP = 1024
OWN = 128
FACTOR = math.sqrt(3.0) * math.sqrt(4.0 * math.pi) / LP * 2.0 ** (-30)


def lane_blocks(values, lane):
    low = lane < 64

    def swap(a, b, width, mask):
        ra = pltpu.roll(a, 128 - width, 1)
        rb = pltpu.roll(b, width, 1)
        return jnp.where(mask, a, rb), jnp.where(mask, ra, b)

    v0, v1, v2, v3 = values
    a0, a2 = swap(v0, v2, 64, low)
    a1, a3 = swap(v1, v3, 64, low)
    even = (lane % 64) < 32
    b0, b1 = swap(a0, a1, 32, even)
    b2, b3 = swap(a2, a3, 32, even)
    return b0, b1, b2, b3


def fourier_kernel(
    coef_ref, out_ref, basis_out,
    coef_v, lhs_v, tab, factors, stage, basis_v, f, got, mean, buf_a, relay, buf_b, buf_c, piece,
    load_sem, out_sem, basis_sem,
    raw_s, raw_r, sa, ra, sb, rb, sc, rc, sd, rd, sf, rf, sg, rg,
):
    member, space = lax.axis_index("member"), lax.axis_index("space")
    z, xl, core = member // 4, (member // 2) % 2, member % 2

    def member_of(z, xl, core):
        return (z * 2 + xl) * 2 + core

    def real(g):
        return min(GO, ORDERS - g * GO)

    loads = [
        pltpu.make_async_copy(
            coef_ref.at[0, :, pl.ds(g * GO, real(g))],
            coef_v.at[:, pl.ds(g * GO, real(g))],
            load_sem.at[g],
        )
        for g in range(GROUPS)
    ]
    for load in loads:
        load.start()

    z_up, z_down = member_of((z + 1) % 4, xl, core), member_of((z + 3) % 4, xl, core)
    x_peer = member_of(z, 1 - xl, core)
    c_peer = member_of(z, xl, 1 - core)
    s_peers = [(space + d) % BANDS for d in range(1, BANDS)]
    barrier = pltpu.get_barrier_semaphore()
    for peer in (z_up, z_down, x_peer, c_peer):
        pl.semaphore_signal(barrier, inc=1, device_id=(peer, space), device_id_type=MESH)
    for peer in s_peers:
        pl.semaphore_signal(barrier, inc=1, device_id=(member, peer), device_id_type=MESH)

    def clear_pads(n, _):
        lhs_v[2, pl.ds(pl.multiple_of(n * MROWS, 8), MROWS), :] = jnp.zeros(
            (MROWS, 128), jnp.float32
        )
        for h in range(2):
            for at in range(LP // 8 * 8, 384, 8):
                tab[h, pl.ds(pl.multiple_of(n * LROWS + at, 8), 8), :] = jnp.zeros(
                    (8, 128), jnp.float32
                )
        return 0

    lax.fori_loop(0, GO, clear_pads, 0)
    for k in range(CHUNKS):
        for s in range(BANDS):
            f[k, s, pl.ds(PIECE, PIECEP - PIECE), :] = jnp.zeros(
                (PIECEP - PIECE, 128), jnp.bfloat16
            )

    row_first = (LON // 2 + 1 - TCOUNT) // 2
    colatitude = (
        math.pi
        * (row_first + lax.broadcasted_iota(jnp.int32, (GO, TCOUNT), 1)).astype(jnp.float32)
        / (LON // 2)
    )
    cosine = jnp.cos(colatitude)
    log_sine = jnp.log(jnp.sin(colatitude))

    def arrange(g, c, i):
        base = c // R * 48 + c % R
        for t in range(3):
            wide = min(128, LP - 128 * t)
            raw = coef_v[c, g * GO + i, :, pl.ds(128 * t, wide)]
            lhs_v[t, pl.ds(i * MROWS + base, 2, stride=RP), pl.ds(0, wide)] = (
                raw.astype(jnp.float32) * FACTOR
            )

    def table(g):
        first = space * ORDERS + g * GO
        order_wide = first + lax.broadcasted_iota(jnp.int32, (GO, TCOUNT), 0)
        order = (first + lax.broadcasted_iota(jnp.int32, (GO, 128), 0)).astype(jnp.float32)
        square = order * order
        degrees = [
            (tile * 128 + lax.broadcasted_iota(jnp.int32, (GO, 128), 1)).astype(jnp.float32)
            for tile in range(3)
        ]
        logs = jnp.zeros((GO, 1), jnp.float32)
        for degree in degrees:
            at_least = jnp.maximum(degree, 1.0)
            term = 0.5 * jnp.log((2.0 * at_least + 1.0) / (2.0 * at_least))
            term = jnp.where((degree >= 1.0) & (degree <= order), term, 0.0)
            logs += jnp.sum(term, axis=1, keepdims=True)
        diag = jnp.exp(
            logs - 0.5 * math.log(4.0 * math.pi) + order_wide.astype(jnp.float32) * log_sine
        )

        def spread(tile, _):
            degree = tile * 128 + lax.broadcasted_iota(jnp.int32, (GO, 128), 1)
            degree = degree.astype(jnp.float32)
            degree_square = degree * degree
            up = jnp.sqrt(
                jnp.maximum(4.0 * degree_square - 1.0, 1.0)
                / jnp.maximum(degree_square - square, 1.0)
            )
            for u in range(128):
                row = pl.multiple_of((tile * 128 + u) * GO, 8)
                factors[pl.ds(row, GO), :] = jnp.broadcast_to(up[:, u : u + 1], (GO, 128))
            return 0

        lax.fori_loop(0, 3, spread, 0)
        loads[g].wait()
        half_order = order_wide[:, :128]

        def block(j, carry, steps=8, channels=True):
            older, newer, down = carry
            for u in range(steps):
                deg = j * 8 + u
                row = pl.multiple_of(deg * GO, 8)
                up = factors[pl.ds(row, GO), :]
                both = up * down
                here = half_order == deg
                fresh = []
                for h in range(2):
                    at = slice(128 * h, 128 * h + 128)
                    seed = jnp.where(here, diag[:, at], 0.0)
                    value = (up * cosine[:, at]) * newer[h] + (seed - both * older[h])
                    tab[h, pl.ds(deg, 8, stride=LROWS), :] = value
                    fresh.append(value)
                older, newer, down = newer, tuple(fresh), 1.0 / up
                if channels:
                    for i in (u % 4 * 2, u % 4 * 2 + 1):
                        if i < real(g):
                            arrange(g, j * 2 + u // 4, i)
            return older, newer, down

        zero = jnp.zeros((GO, 128), jnp.float32)
        carry = ((zero, zero), (zero, zero), zero)
        carry = lax.fori_loop(0, CH // 2, block, carry)
        carry = lax.fori_loop(
            CH // 2, LP // 8, functools.partial(block, channels=False), carry
        )
        block(LP // 8, carry, steps=LP % 8, channels=False)

    lane = lax.broadcasted_iota(jnp.int32, (RP * 2, 128), 1)

    def orders_of(g):
        k, at_group = g // PER, g % PER * GR

        def one(n, _):
            for i in (2 * n, 2 * n + 1):
                row = pl.multiple_of(i * MROWS, 8)
                lhs = jnp.concatenate(
                    [lhs_v[t, pl.ds(row, MROWS), :].astype(jnp.bfloat16) for t in range(3)],
                    axis=1,
                )
                row = pl.multiple_of(i * LROWS, 8)
                rhs = jnp.concatenate(
                    [tab[h, pl.ds(row, 384), :].astype(jnp.bfloat16) for h in range(2)], axis=1
                )
                out = jnp.dot(lhs, rhs, preferred_element_type=jnp.float32)
                for h in range(2):
                    parts = [
                        out[48 * q : 48 * q + 48, 128 * h : 128 * h + 128] for q in range(Q)
                    ]
                    for b, part in enumerate(lane_blocks(parts, lane)):
                        s = 4 * h + b
                        for a in range(6):
                            stage[pl.ds((s * 48 + 8 * a) * GO + i, 8, stride=GO), :] = part[
                                8 * a : 8 * a + 8
                            ]
            return 0

        if real(g) < GO:

            def clear_stage(n, _):
                for i in range(real(g), GO):
                    stage[pl.ds(n * 8 * GO + i, 8, stride=GO), :] = jnp.zeros(
                        (8, 128), jnp.float32
                    )
                return 0

            lax.fori_loop(0, BANDS * 48 // 8, clear_stage, 0)
        lax.fori_loop(0, real(g) // 2, one, 0)

        def pack(n, _):
            s = n // 3
            for u in range(7):
                r = n % 3 * 7 + u
                first = stage[pl.ds(pl.multiple_of((s * 48 + r) * GO, 8), GO), :]
                second = stage[pl.ds(pl.multiple_of((s * 48 + RP + r) * GO, 8), GO), :]
                both = jnp.concatenate([first, second], axis=0).astype(jnp.bfloat16)
                f[k, s, pl.ds(pl.multiple_of(at_group + r * 2 * GO, 16), 2 * GO), :] = both
            return 0

        lax.fori_loop(0, BANDS * 3, pack, 0)

    def remote(src, dst, ss, rs, device):
        return pltpu.make_async_remote_copy(
            src_ref=src, dst_ref=dst, send_sem=ss, recv_sem=rs,
            device_id=device, device_id_type=MESH,
        )

    half = PIECEP // 2
    mine = pl.multiple_of(core * half, 16)
    other = pl.multiple_of((1 - core) * half, 16)
    in_half = pl.multiple_of(z * OWN, 16)
    own_row = pl.multiple_of(core * half + z * OWN, 16)

    def pair_sum(k):
        return remote(
            f.at[k, :, pl.ds(other, half)], buf_a.at[k], sa.at[k], ra.at[k], (c_peer, space)
        )

    def z_sums(k):
        def rows_of(place, at, size):
            row = pl.multiple_of(place * OWN + at, 16)
            return buf_a.at[k, :, pl.ds(row, size)]

        far = (z + 2) % 4
        first = [
            remote(
                rows_of(far, 0, OWN // 2), relay.at[k, 0], sb.at[k, 0], rb.at[k, 0],
                (z_up, space),
            ),
            remote(
                rows_of(far, OWN // 2, OWN // 2), relay.at[k, 1], sb.at[k, 1], rb.at[k, 1],
                (z_down, space),
            ),
        ]
        second = [
            remote(
                rows_of((z + 1) % 4, 0, OWN), buf_b.at[k, 0], sb.at[k, 2], rb.at[k, 2],
                (z_up, space),
            ),
            remote(
                rows_of((z + 3) % 4, 0, OWN), buf_b.at[k, 1], sb.at[k, 3], rb.at[k, 3],
                (z_down, space),
            ),
        ]
        return first, second

    def add_relay(k):
        def one(s, _):
            for n, place, at in ((0, (z + 1) % 4, 0), (1, (z + 3) % 4, OWN // 2)):
                row = pl.multiple_of(place * OWN + at, 16)
                total = buf_a[k, s, pl.ds(row, OWN // 2), :].astype(jnp.float32)
                total += relay[k, n, s].astype(jnp.float32)
                buf_a[k, s, pl.ds(row, OWN // 2), :] = total.astype(jnp.bfloat16)
            return 0

        lax.fori_loop(0, BANDS, one, 0)

    def x_sum(k):
        return remote(piece.at[k], buf_c.at[k], sc.at[k], rc.at[k], (x_peer, space))

    def means_out(k):
        return [
            remote(
                buf_c.at[k, (space + d) % BANDS], mean.at[k, d, pl.ds(own_row, OWN)],
                sd.at[k, d - 1], rd.at[k, d - 1], (member, (space + d) % BANDS),
            )
            for d in range(1, BANDS)
        ]

    def z_gather(k):
        def rows_of(place, at, size):
            row = pl.multiple_of(core * half + place * OWN + at, 16)
            return mean.at[k, :, pl.ds(row, size)]

        first = [
            remote(rows_of(z, 0, OWN), rows_of(z, 0, OWN), sf.at[k, n], rf.at[k, n], device)
            for n, device in enumerate(((z_up, space), (z_down, space)))
        ]
        second = [
            remote(
                rows_of((z + 3) % 4, 0, OWN // 2), rows_of((z + 3) % 4, 0, OWN // 2),
                sf.at[k, 2], rf.at[k, 2], (z_up, space),
            ),
            remote(
                rows_of((z + 1) % 4, OWN // 2, OWN // 2),
                rows_of((z + 1) % 4, OWN // 2, OWN // 2),
                sf.at[k, 3], rf.at[k, 3], (z_down, space),
            ),
        ]
        return first, second

    def core_gather(k):
        return remote(
            mean.at[k, :, pl.ds(mine, half)], mean.at[k, :, pl.ds(mine, half)],
            sg.at[k], rg.at[k], (c_peer, space),
        )

    def raw(k, part, at, size):
        return [
            remote(
                f.at[k, (space + d) % BANDS, pl.ds(at, size)], got.at[k, d, pl.ds(at, size)],
                raw_s.at[part, d - 1], raw_r.at[part, d - 1],
                (member, (space + d) % BANDS),
            )
            for d in range(1, BANDS)
        ]

    def begin(copies):
        for copy in copies:
            copy.start()

    def finish(copies):
        for copy in copies:
            copy.wait()

    def add_pair(k):
        def one(n, _):
            s, at = n // 4, pl.multiple_of(n % 4 * OWN, 16)
            total = buf_a[k, s, pl.ds(at, OWN), :].astype(jnp.float32)
            total += f[k, s, pl.ds(mine + at, OWN), :].astype(jnp.float32)
            buf_a[k, s, pl.ds(at, OWN), :] = total.astype(jnp.bfloat16)
            return 0

        lax.fori_loop(0, BANDS * 4, one, 0)

    def add_four(k):
        def one(s, _):
            total = buf_a[k, s, pl.ds(in_half, OWN), :].astype(jnp.float32)
            for d in range(2):
                total += buf_b[k, d, s].astype(jnp.float32)
            piece[k, s] = total.astype(jnp.bfloat16)
            return 0

        lax.fori_loop(0, BANDS, one, 0)

    def add_two(k):
        def one(s, _):
            total = buf_c[k, s].astype(jnp.float32) + piece[k, s].astype(jnp.float32)
            buf_c[k, s] = (total * (1.0 / 16.0)).astype(jnp.bfloat16)
            return 0

        lax.fori_loop(0, BANDS, one, 0)
        mean[k, 0, pl.ds(own_row, OWN), :] = buf_c[k, space]

    def outs(k, d):
        return pltpu.make_async_copy(
            got.at[k, d], out_ref.at[(space + BANDS - d) % BANDS, k], out_sem.at[k, d]
        )

    def centre(k):
        for d in range(BANDS):

            def one(n, _):
                at = pl.multiple_of(n * 112, 16)
                block = f[k, space, pl.ds(at, 112), :] if d == 0 else got[k, d, pl.ds(at, 112), :]
                block = block.astype(jnp.float32) - mean[k, d, pl.ds(at, 112), :].astype(
                    jnp.float32
                )
                got[k, d, pl.ds(at, 112), :] = block.astype(jnp.bfloat16)
                return 0

            lax.fori_loop(0, 9, one, 0)
            outs(k, d).start()

    column = lax.broadcasted_iota(jnp.int32, (GO, LON), 1).astype(jnp.float32)
    index = lax.broadcasted_iota(jnp.int32, (GO, LON), 0)

    def basis():
        def one(n, _):
            slot = n % GROUPS * GO + index
            order = n // GROUPS * ORDERS + slot
            product = order.astype(jnp.float32) * column
            turns = jnp.floor((product + 0.5) * (1.0 / LON))
            angle = 2.0 * math.pi / LON * (product - turns * LON)
            weight = jnp.where(order == 0, 1.0, math.sqrt(2.0))
            weight = jnp.where(slot < ORDERS, weight, 0.0)
            both = jnp.concatenate(
                [weight * jnp.cos(angle), weight * jnp.sin(angle)], axis=0
            )
            basis_v[pl.ds(pl.multiple_of(n * 2 * GO, 16), 2 * GO), :] = both.astype(
                jnp.bfloat16
            )
            return 0

        lax.fori_loop(0, BANDS * GROUPS, one, 0)

    def group(g):
        table(g)
        orders_of(g)

    def raw_group(part, g, at=0, size=GR):
        return raw(g // PER, part, g % PER * GR + at, size)

    a0, a1 = pair_sum(0), pair_sum(1)
    (r0, b0), (r1, b1) = z_sums(0), z_sums(1)
    c0, c1 = x_sum(0), x_sum(1)
    d0, d1 = means_out(0), means_out(1)
    (f0, h0), (f1, h1) = z_gather(0), z_gather(1)
    g0, g1 = core_gather(0), core_gather(1)
    pieces = (
        (0, 0, GR), (1, 0, GR), (2, 0, GR), (3, 0, 224),
        (3, 224, 64), (3, 288, 48), (4, 0, 64), (4, 64, 64), (4, 128, GR - 128), (5, 0, GR),
    )
    raws = [raw_group(n, *piece) for n, piece in enumerate(pieces)]

    group(0)
    pl.semaphore_wait(barrier, 4 + BANDS - 1)
    begin(raws[0])
    group(1)
    begin(raws[1])
    group(2)
    a0.start()
    begin(raws[2])
    table(3)
    a0.wait()
    add_pair(0)
    begin(r0)
    orders_of(3)
    finish(r0)
    add_relay(0)
    begin(b0)
    begin(raws[3])
    group(4)
    group(5)
    a1.start()
    finish(b0)
    add_four(0)
    c0.start()
    begin(raws[4])
    a1.wait()
    add_pair(1)
    begin(r1)
    finish(r1)
    add_relay(1)
    begin(b1)
    c0.wait()
    add_two(0)
    begin(d0)
    begin(raws[5])
    begin(raws[6])
    finish(d0)
    begin(f0)
    finish(b1)
    add_four(1)
    c1.start()
    begin(raws[7])
    finish(f0)
    begin(h0)
    c1.wait()
    add_two(1)
    begin(d1)
    begin(raws[8])
    begin(raws[9])
    finish(h0)
    g0.start()
    finish(d1)
    begin(f1)
    finish(f1)
    begin(h1)
    basis()
    basis_copy = pltpu.make_async_copy(basis_v, basis_out, basis_sem)
    basis_copy.start()
    finish(raws[0])
    finish(raws[1])
    finish(raws[2])
    g0.wait()
    centre(0)
    finish(h1)
    g1.start()
    for copies in raws[3:]:
        finish(copies)
    g1.wait()
    centre(1)
    basis_copy.wait()
    for k in range(CHUNKS):
        for d in range(BANDS):
            outs(k, d).wait()


def fourier_blocks(coefficients):
    sem = pltpu.SemaphoreType.DMA
    bf = jnp.bfloat16
    basis = (BANDS * GROUPS * 2 * GO, LON)
    return pl.pallas_call(
        fourier_kernel,
        name="fourier_blocks",
        out_shape=[
            jax.ShapeDtypeStruct((BANDS, CHUNKS, PIECE, 128), bf),
            jax.ShapeDtypeStruct(basis, bf),
        ],
        in_specs=[pl.BlockSpec(memory_space=pl.ANY)],
        out_specs=[pl.BlockSpec(memory_space=pl.ANY)] * 2,
        scratch_shapes=[
            pltpu.VMEM((CH, ORDERS, 2, LP), jnp.int32),
            pltpu.VMEM((3, GO * MROWS, 128), jnp.float32),
            pltpu.VMEM((2, GO * LROWS, 128), jnp.float32),
            pltpu.VMEM((384 * GO, 128), jnp.float32),
            pltpu.VMEM((BANDS * 48 * GO, 128), jnp.float32),
            pltpu.VMEM(basis, bf),
            pltpu.VMEM((CHUNKS, BANDS, PIECEP, 128), bf),
            pltpu.VMEM((CHUNKS, BANDS, PIECE, 128), bf),
            pltpu.VMEM((CHUNKS, BANDS, PIECEP, 128), bf),
            pltpu.VMEM((CHUNKS, BANDS, PIECEP // 2, 128), bf),
            pltpu.VMEM((CHUNKS, 2, BANDS, OWN // 2, 128), bf),
            pltpu.VMEM((CHUNKS, 2, BANDS, OWN, 128), bf),
            pltpu.VMEM((CHUNKS, BANDS, OWN, 128), bf),
            pltpu.VMEM((CHUNKS, BANDS, OWN, 128), bf),
            sem((GROUPS,)), sem((CHUNKS, BANDS)), sem,
            sem((10, 7)), sem((10, 7)),
            sem((2,)), sem((2,)),
            sem((2, 4)), sem((2, 4)),
            sem((2,)), sem((2,)),
            sem((2, 7)), sem((2, 7)),
            sem((2, 4)), sem((2, 4)),
            sem((2,)), sem((2,)),
        ],
        compiler_params=pltpu.CompilerParams(
            collective_id=1, has_side_effects=True, vmem_limit_bytes=63 * 2**20
        ),
    )(coefficients)


RB = 7


def synthesis_kernel(f_ref, basis_ref, scale_ref, weather_ref, out_ref):
    step = pl.program_id(0)
    rows = []
    for r in range(RB):
        x = f_ref[:, :, r].reshape(BANDS * GROUPS * 2 * GO, 128)
        rows.append(x.T)
    lhs = jnp.concatenate(rows, axis=0)
    noise = jnp.dot(lhs, basis_ref[...], preferred_element_type=jnp.float32)
    for r in range(RB):
        for q in range(Q):
            scale = scale_ref[q * R + step * RB + r]
            at = (r * Q + q) * 32
            out_ref[0, q, r] = (
                weather_ref[0, q, r].astype(jnp.float32) + scale * noise[at : at + 32]
            ).astype(jnp.bfloat16)


def synthesis(fourier, basis, scale, weather):
    fourier = fourier.reshape(BANDS, GROUPS, R, 2 * GO, 128)
    rows = weather.shape[2]
    weather = weather.reshape(1, Q, R, rows, LON)
    block = pl.BlockSpec((1, Q, RB, rows, LON), lambda i: (0, 0, i, 0, 0))
    out = pl.pallas_call(
        synthesis_kernel,
        name="synthesis",
        grid=(R // RB,),
        out_shape=jax.ShapeDtypeStruct(weather.shape, jnp.bfloat16),
        in_specs=[
            pl.BlockSpec((BANDS, GROUPS, RB, 2 * GO, 128), lambda i: (0, 0, i, 0, 0)),
            pl.BlockSpec(basis.shape, lambda i: (0, 0)),
            pl.BlockSpec(memory_space=pltpu.SMEM),
            block,
        ],
        out_specs=block,
        compiler_params=pltpu.CompilerParams(
            dimension_semantics=("arbitrary",), vmem_limit_bytes=63 * 2**20
        ),
    )(fourier, basis, scale, weather)
    return out.reshape(1, CH, rows, LON)


def local(weather, coefficients, channel_scale):
    centred, basis = fourier_blocks(coefficients.transpose(0, 1, 3, 2, 4))
    return synthesis(centred, basis, channel_scale, weather)


def solution(mesh):
    return jax.shard_map(
        local,
        mesh=mesh,
        in_specs=(P("member", None, "space", None), P("member", None, None, "space", None), P()),
        out_specs=P("member", None, "space", None),
        check_vma=False,
    )
```
